32 devices in a mesh: expert: 8 (over y, x, core), shard: 4 (over z).
Axes of the slice: x: 2, y: 2, z: 4, core: 2. Of those that a mesh axis runs over, the one named last changes fastest.
Arguments:
- w_gate: float32 [64, 2048, 1024], P('expert', 'shard'), may hold values from -0.1875 to 0.1875
- avg_gate: float32 [64, 2048, 1024], P('expert', 'shard'), may hold values from -0.125 to 0.125
- w_up: float32 [64, 2048, 1024], P('expert', 'shard'), may hold values from -0.1875 to 0.1875
- avg_up: float32 [64, 2048, 1024], P('expert', 'shard'), may hold values from -0.125 to 0.125
- mix_share: float32 [64], P('expert'), may hold values from 0.2 to 0.8
- router_weight: float32 [2048, 64], P('shard', 'expert'), may hold values from -0.125 to 0.125
- router_gain: float32 [2048], P('shard'), may hold values from 0.25 to 1.75
Outputs:
- serve_gate: bfloat16 [64, 2048, 1024], P('expert')
- serve_up: bfloat16 [64, 2048, 1024], P('expert')
- scale_gate: float32 [64, 1024], P('expert')
- scale_up: float32 [64, 1024], P('expert')
- serve_router: bfloat16 [2048, 64], replicated
The draws below stay inside these ranges and needn't reach their ends.
All inputs are finite; a program needn't handle non-finite values.
Results may differ from the reference program's by a relative error of at most 0.001.
Values may be sent and summed in bfloat16 or wider, within the bound.
A program may use at most 256 MiB of HBM per device.

```python
import jax
import jax.numpy as jnp
from jax import lax

EXPERTS = 64
D_MODEL = 2048
D_EXPERT = 1024


def with_spikes(result, own_key, source, target, parts, factor):
    def block_of(position):
        return (jnp.arange(result.shape[position]) // (result.shape[position] // parts)).reshape((-1,) + (1,) * (result.ndim - 1 - position))

    first = jax.random.permutation(own_key, parts)[block_of(target)]
    second = (block_of(target) + parts // 2) % parts
    return jnp.where((block_of(source) == first) | (block_of(source) == second), factor * result, result)


def level_of(stream_key, dims, shards, low, top_value):
    def one(dim, parts):
        steps = jax.random.uniform(jax.random.fold_in(jax.random.fold_in(stream_key, 6), dim), (parts,), jnp.float32, low / len(shards), top_value / len(shards))
        return jnp.repeat(jnp.exp(steps), dims[dim] // parts).reshape((-1,) + (1,) * (len(dims) - dim - 1))

    gain = one(*shards[0])
    for cut in shards[1:]:
        gain = gain * one(*cut)
    return gain


def normal_values(own_key, extent, width, reach, pieces=(), kind=jnp.bfloat16):
    level = level_of(own_key, extent, pieces, -0.22, 0.18) if pieces else 1.0
    values = jax.random.normal(own_key, extent, jnp.float32) * width * level
    return jnp.minimum(jnp.maximum(values, -reach), reach).astype(kind)


def noise_with(stream_key, extent, scale, bound, shards, heavy, dtype=jnp.bfloat16):
    values = scale * jax.random.normal(stream_key, extent, jnp.float32)
    if shards:
        values = values * level_of(stream_key, extent, shards, -0.22, 0.18)
    return jnp.clip(with_spikes(values, jax.random.fold_in(stream_key, 3), *heavy), -bound, bound).astype(dtype)


def setup_inputs(seed: int = 0) -> dict:
    key_of = jax.random.split(jax.random.key(seed), 8)
    return {
        "w_gate": noise_with(key_of[0], (EXPERTS, D_MODEL, D_EXPERT), D_MODEL ** -0.5, 0.1875, ((0, 8), (1, 4)), (1, 2, 4, 2.0), jnp.float32),
        "avg_gate": normal_values(key_of[1], (EXPERTS, D_MODEL, D_EXPERT), D_MODEL ** -0.5, 0.125, ((0, 8), (1, 4)), jnp.float32),
        "w_up": noise_with(key_of[2], (EXPERTS, D_MODEL, D_EXPERT), D_MODEL ** -0.5, 0.1875, ((0, 8), (1, 4)), (1, 2, 4, 2.0), jnp.float32),
        "avg_up": normal_values(key_of[3], (EXPERTS, D_MODEL, D_EXPERT), D_MODEL ** -0.5, 0.125, ((0, 8), (1, 4)), jnp.float32),
        "mix_share": jnp.clip(0.2 + 0.6 * jax.random.uniform(key_of[4], (EXPERTS,), jnp.float32) ** level_of(key_of[4], (EXPERTS,), ((0, 8),), -0.2, 0.2), 0.2, 0.8),
        "router_weight": normal_values(key_of[5], (D_MODEL, EXPERTS), D_MODEL ** -0.5, 0.125, ((0, 4), (1, 8)), jnp.float32),
        "router_gain": jnp.clip(1.0 + 0.15 * jax.random.normal(key_of[6], (D_MODEL,), jnp.float32), 0.25, 1.75),
    }


def reference(w_gate, avg_gate, w_up, avg_up, mix_share, router_weight, router_gain):
    fresh_gate = mix_share[:, None, None] * w_gate + (1.0 - mix_share[:, None, None]) * avg_gate
    fresh_up = mix_share[:, None, None] * w_up + (1.0 - mix_share[:, None, None]) * avg_up
    scale_gate = jnp.sqrt(lax.optimization_barrier(jnp.sum(fresh_gate * fresh_gate, axis=1)))
    serve_gate = (fresh_gate / jnp.expand_dims(scale_gate, 1)).astype(jnp.bfloat16)
    scale_up = jnp.sqrt(lax.optimization_barrier(jnp.sum(fresh_up * fresh_up, axis=1)))
    serve_up = (fresh_up / jnp.expand_dims(scale_up, 1)).astype(jnp.bfloat16)
    serve_router = (router_weight * router_gain[:, None]).astype(jnp.bfloat16)
    return (serve_gate, serve_up, scale_gate, scale_up, serve_router)
```

```python
import functools

import jax
import jax.numpy as jnp
from jax import lax
from jax.experimental import pallas as pl
from jax.experimental.pallas import tpu as pltpu
from jax.sharding import PartitionSpec as P

MESH = pl.DeviceIdType.MESH
SLOTS = 4
ROWS = 16
HEAD_PARTS = 4


def kernel(
    ns, ne, experts, rows, cols, ahead,
    mix_ref, wg_ref, ag_ref, wu_ref, au_ref, router_ref, gain_ref,
    og_ref, ou_ref, sg_ref, su_ref, bundle_ref, table_ref,
    fresh, other, narrow, first_sums, head, tail, scale, mix_s, weight, gain, column,
    w_sem, a_sem, first_sem, small_sem, local_sem, recv_sem, right_sem, left_sem,
    first_send, first_recv, head_send, head_recv, tail_send, tail_recv,
    column_send, column_recv, table_send, table_recv, own_sem,
):
    z, me = lax.axis_index("shard"), lax.axis_index("expert")
    n = 2 * experts
    half = ns // 2
    firsts, seconds, outs = (wg_ref, wu_ref), (ag_ref, au_ref), (og_ref, ou_ref)
    scales = (sg_ref, su_ref)
    lead, follow = pl.ds(0, ahead), pl.ds(ahead, cols - ahead)

    first_w = pltpu.make_async_copy(wg_ref.at[0, :, lead], fresh.at[0, :, lead], first_sem.at[0])
    first_a = pltpu.make_async_copy(ag_ref.at[0, :, lead], other.at[0, :, lead], first_sem.at[1])
    rest_w = pltpu.make_async_copy(wg_ref.at[0, :, follow], fresh.at[0, :, follow], w_sem.at[0])
    rest_a = pltpu.make_async_copy(ag_ref.at[0, :, follow], other.at[0, :, follow], a_sem.at[0])
    get_mix = pltpu.make_async_copy(mix_ref, mix_s, small_sem.at[0])
    get_weight = pltpu.make_async_copy(router_ref, weight, small_sem.at[1])
    get_gain = pltpu.make_async_copy(gain_ref, gain, small_sem.at[2])

    first_w.start()
    first_a.start()
    get_mix.start()

    barrier = pltpu.get_barrier_semaphore()
    for k in range(1, ns):
        pl.semaphore_signal(barrier, inc=1, device_id={"shard": lax.rem(z + k, ns)}, device_id_type=MESH)

    def greet(k, carry):
        pl.semaphore_signal(barrier, inc=1, device_id={"expert": lax.rem(me + k, ne)}, device_id_type=MESH)
        return carry

    lax.fori_loop(1, ne, greet, 0)
    get_weight.start()
    get_gain.start()

    def w_copy(e, which):
        c = 2 * e + which
        return pltpu.make_async_copy(firsts[which].at[e], fresh.at[c], w_sem.at[c])

    def a_copy(e, which):
        slot = lax.rem(2 * e + which, SLOTS)
        return pltpu.make_async_copy(seconds[which].at[e], other.at[slot], a_sem.at[slot])

    def load(e, which):
        w_copy(e, which).start()
        a_copy(e, which).start()

    def place(e, which, j):
        return outs[which].at[e, pl.ds(pl.multiple_of(j * rows, rows), rows), :]

    def local_copy(e, which):
        c = 2 * e + which
        return pltpu.make_async_copy(narrow.at[c], place(e, which, z), local_sem.at[c])

    def hop(src, dst, step, d, c, j):
        send_sem = right_sem if step > 0 else left_sem
        return pltpu.make_async_remote_copy(
            src_ref=src, dst_ref=dst, send_sem=send_sem.at[d, c], recv_sem=recv_sem.at[j, c],
            device_id={"shard": z + step}, device_id_type=MESH,
        )

    def send_on(e, which, step, d):
        c = 2 * e + which
        j = z - step * d
        spot = place(e, which, j)
        return hop(narrow.at[c] if d == 0 else spot, spot, step, d, c, j)

    def send_part(part, step):
        spot = place(0, 0, z)
        return hop(narrow.at[0, :, part], spot.at[:, part], step, 0, 0, z)

    def arrival(e, which, j):
        c = 2 * e + which
        return pltpu.make_async_copy(place(e, which, j), place(e, which, j), recv_sem.at[j, c])

    def plain_at(device, j):
        return jnp.where(device < half, j == 0, j == ns - 1)

    def slot_at(device, j):
        return jnp.where(device < half, j - 1, j)

    def last_copy(step, d, from_plain, to_plain):
        j = z - step * d
        spot = place(experts - 1, 1, j)
        src = narrow.at[n - 1] if d == 0 else spot if from_plain else bundle_ref.at[slot_at(z, j)]
        dst = spot if to_plain else bundle_ref.at[slot_at(z + step, j)]
        return hop(src, dst, step, d, n - 1, j)

    def last_goes(step, d):
        j = z - step * d
        return (z + step >= 1) & (z + step <= ns - 2) & (j >= 0) & (j <= ns - 1)

    def send_last(step, d):
        j = z - step * d
        goes, here, there = last_goes(step, d), plain_at(z, j), plain_at(z + step, j)
        for from_plain in (False, True):
            if d == 0 and from_plain:
                continue
            for to_plain in (False, True):
                fits = goes & (there if to_plain else jnp.logical_not(there))
                if d > 0:
                    fits = fits & (here if from_plain else jnp.logical_not(here))
                pl.when(fits)(lambda: last_copy(step, d, from_plain, to_plain).start())

    def last_sent(step, d):
        return hop(narrow.at[n - 1], narrow.at[n - 1], step, d, n - 1, z)

    inner = (z > 0) & (z < ns - 1)
    own_inner = pltpu.make_async_copy(narrow.at[n - 1], bundle_ref.at[slot_at(z, z)], local_sem.at[n - 1])
    own_outer = local_copy(experts - 1, 1)

    def sums_to(part, send, recv, k):
        return pltpu.make_async_remote_copy(
            src_ref=part.at[z], dst_ref=part.at[z], send_sem=send.at[k], recv_sem=recv.at[z],
            device_id={"shard": lax.rem(z + k, ns)}, device_id_type=MESH,
        )

    def sums_from(part, recv, k):
        j = lax.rem(z + k, ns)
        return pltpu.make_async_copy(part.at[j], part.at[j], recv.at[j])

    def exchange(part, send, recv):
        for k in range(1, ns):
            sums_to(part, send, recv, k).start()

    def collect(part, recv):
        for k in range(1, ns):
            sums_from(part, recv, k).wait()

    def column_to(k):
        return pltpu.make_async_remote_copy(
            src_ref=column.at[z], dst_ref=column.at[z], send_sem=column_send.at[k], recv_sem=column_recv.at[z],
            device_id={"shard": lax.rem(z + k, ns)}, device_id_type=MESH,
        )

    def column_from(k):
        j = lax.rem(z + k, ns)
        return pltpu.make_async_copy(column.at[j], column.at[j], column_recv.at[j])

    def table_to(k):
        return pltpu.make_async_remote_copy(
            src_ref=column, dst_ref=table_ref.at[me], send_sem=table_send.at[k], recv_sem=table_recv.at[me],
            device_id={"expert": lax.rem(me + k, ne)}, device_id_type=MESH,
        )

    def table_from(k):
        j = lax.rem(me + k, ne)
        return pltpu.make_async_copy(table_ref.at[j], table_ref.at[j], table_recv.at[j])

    own_table = pltpu.make_async_copy(column, table_ref.at[me], own_sem.at[0])
    put_scales = [pltpu.make_async_copy(scale.at[i], scales[i], own_sem.at[1 + i]) for i in range(2)]

    def mix(c, e, slot, part, row, lo=0, hi=cols, height=ROWS):
        span = pl.ds(lo, hi - lo)
        share = mix_s[e]
        rest = 1.0 - share

        def step(i, acc):
            r = pl.ds(pl.multiple_of(i * height, height), height)
            value = share * fresh[c, r, span] + rest * other[slot, r, span]
            fresh[c, r, span] = value
            square = value * value
            for k in range(0, height, 8):
                acc = acc + square[k : k + 8]
            return acc

        acc = lax.fori_loop(0, rows // height, step, jnp.zeros((8, hi - lo), jnp.float32), unroll=2)
        part[z, pl.ds(row, 1), span] = jnp.sum(acc, axis=0, keepdims=True)

    def divide(c, e, which, part, row, lo=0, hi=cols, height=ROWS):
        span = pl.ds(lo, hi - lo)
        total = part[0, pl.ds(row, 1), span]
        for j in range(1, ns):
            total = total + part[j, pl.ds(row, 1), span]
        root = jnp.sqrt(total)
        scale[which, pl.ds(e, 1), span] = root
        wide = jnp.broadcast_to(root, (8, hi - lo))
        wide = jnp.concatenate([wide] * (height // 8), axis=0)

        def step(i, carry):
            r = pl.ds(pl.multiple_of(i * height, height), height)
            narrow[c, r, span] = (fresh[c, r, span] / wide).astype(jnp.bfloat16)
            return carry

        lax.fori_loop(0, rows // height, step, 0, unroll=2)

    def both_ways(go):
        pl.when(z > 0)(lambda: go(-1))
        pl.when(z < ns - 1)(lambda: go(1))

    def finish(e, which, part, row):
        divide(2 * e + which, e, which, part, row)

        def send():
            both_ways(lambda step: send_on(e, which, step, 0).start())
            local_copy(e, which).start()

        if which == 0:
            send()
        else:
            pl.when(e < experts - 1)(send)

    def settle_piece(e, which):
        w_copy(e, which).wait()
        a_copy(e, which).wait()

    def slot_of(e, which):
        return lax.rem(2 * e + which, SLOTS)

    def refill(e, which):
        @pl.when(e + SLOTS // 2 < experts)
        def _():
            load(e + SLOTS // 2, which)

    get_mix.wait()
    first_w.wait()
    first_a.wait()
    rest_w.start()
    rest_a.start()
    load(0, 1)
    mix(0, 0, 0, first_sums, 0, 0, ahead, 4 * ROWS)
    pl.semaphore_wait(barrier, ns - 1 + ne - 1)
    exchange(first_sums, first_send, first_recv)
    rest_w.wait()
    rest_a.wait()
    if experts > 1:
        load(1, 0)
        load(1, 1)
    mix(0, 0, 0, head, 0, ahead, cols)
    refill(0, 0)
    collect(first_sums, first_recv)
    divide(0, 0, 0, first_sums, 0, 0, ahead, 4 * ROWS)
    both_ways(lambda step: send_part(lead, step).start())
    settle_piece(0, 1)
    mix(1, 0, 1, head, 1)
    refill(0, 1)
    exchange(head, head_send, head_recv)

    get_weight.wait()
    get_gain.wait()
    column[z] = (weight[...] * gain[...]).astype(jnp.bfloat16)
    if experts > 1:
        settle_piece(1, 0)
        mix(2, 1, 2, tail, 0)
        refill(1, 0)
    collect(head, head_recv)
    divide(0, 0, 0, head, 0, ahead, cols)
    both_ways(lambda step: send_part(follow, step).start())
    local_copy(0, 0).start()
    finish(0, 1, head, 1)
    for k in range(1, ns):
        column_to(k).start()
    if experts > 1:
        settle_piece(1, 1)
        mix(3, 1, 3, tail, 1)
        refill(1, 1)

        def more(e, carry):
            for which in range(2):
                settle_piece(e, which)
                mix(2 * e + which, e, slot_of(e, which), tail, 2 * (e - 1) + which)
                refill(e, which)
            return carry

        lax.fori_loop(2, experts, more, 0)
        exchange(tail, tail_send, tail_recv)
        collect(tail, tail_recv)

        def rest(e, carry):
            for which in range(2):
                finish(e, which, tail, 2 * (e - 1) + which)
            return carry

        lax.fori_loop(1, experts, rest, 0)

    for step in (-1, 1):
        send_last(step, 0)
    pl.when(inner)(lambda: own_inner.start())
    pl.when(jnp.logical_not(inner))(lambda: own_outer.start())
    for put in put_scales:
        put.start()

    for k in range(1, ns):
        column_from(k).wait()
    own_table.start()

    def spread(k, carry):
        table_to(k).start()
        return carry

    lax.fori_loop(1, ne, spread, 0)

    def each(step):
        def both(e, carry):
            step(e, 0)
            pl.when(e < experts - 1)(lambda: step(e, 1))
            return carry

        lax.fori_loop(0, experts, both, 0)

    def land(e, which, d):
        @pl.when(z >= d)
        def _():
            arrival(e, which, z - d).wait()

        @pl.when(z + d < ns)
        def _():
            arrival(e, which, z + d).wait()

    for d in range(1, ns - 1):
        def pass_on(e, which, d=d):
            land(e, which, d)

            @pl.when((z + d < ns) & (z > 0))
            def _():
                send_on(e, which, -1, d).start()

            @pl.when((z >= d) & (z < ns - 1))
            def _():
                send_on(e, which, 1, d).start()

        each(pass_on)
        pl.when(inner)(lambda: land(experts - 1, 1, d))
        for step in (-1, 1):
            send_last(step, d)

    own_outer.wait()
    for put in put_scales:
        put.wait()
    own_table.wait()

    def settle(k, carry):
        table_to(k).wait_send()
        table_from(k).wait()
        return carry

    lax.fori_loop(1, ne, settle, 0)
    for k in range(1, ns):
        column_to(k).wait_send()
        sums_to(first_sums, first_send, first_recv, k).wait_send()
        sums_to(head, head_send, head_recv, k).wait_send()
        if experts > 1:
            sums_to(tail, tail_send, tail_recv, k).wait_send()
    for d in range(ns - 1):
        for step in (-1, 1):
            pl.when(last_goes(step, d))(lambda: last_sent(step, d).wait_send())

    def drain(e, which):
        local_copy(e, which).wait()
        for d in range(ns - 1):
            @pl.when((z + d < ns) & (z > 0))
            def _():
                send_on(e, which, -1, d).wait_send()

            @pl.when((z >= d) & (z < ns - 1))
            def _():
                send_on(e, which, 1, d).wait_send()

    each(drain)
    each(lambda e, which: land(e, which, ns - 1))


def shard_in(slot, ns):
    z = lax.axis_index("shard")
    return jnp.where(z < ns // 2, slot + 1, slot)


def move_kernel(src_ref, dst_ref):
    dst_ref[...] = src_ref[...]


def move(raw):
    block = pl.BlockSpec((1,) + raw.shape[1:], lambda i: (i, 0, 0))
    return pl.pallas_call(
        move_kernel,
        grid=(raw.shape[0],),
        out_shape=jax.ShapeDtypeStruct(raw.shape, raw.dtype),
        in_specs=[block],
        out_specs=block,
        compiler_params=pltpu.CompilerParams(vmem_limit_bytes=32 * 1024 * 1024),
        cost_estimate=pl.CostEstimate(flops=0, bytes_accessed=2 * raw.size * raw.dtype.itemsize, transcendentals=0),
    )(raw)


def move_all_kernel(ns, rows, raw_ref, bundle_ref, *refs):
    count = len(refs) // 2
    dst_ref, smalls, copies = refs[count], refs[:count], refs[count + 1 :]
    dst_ref[...] = raw_ref[...]
    z = lax.axis_index("shard")

    @pl.when(pl.program_id(0) == 0)
    def _():
        for small, copy in zip(smalls, copies):
            copy[...] = small[...]

    @pl.when((pl.program_id(0) == pl.num_programs(0) - 1) & (z > 0) & (z < ns - 1))
    def _():
        for slot in range(ns - 1):
            at = pl.multiple_of(shard_in(slot, ns) * rows, rows)
            dst_ref[0, pl.ds(at, rows), :] = bundle_ref[slot]


def move_all(ns, raw, bundle, smalls):
    block = pl.BlockSpec((1,) + raw.shape[1:], lambda i: (i, 0, 0))

    def whole(x):
        return pl.BlockSpec(x.shape, lambda i: (0,) * x.ndim)

    return pl.pallas_call(
        functools.partial(move_all_kernel, ns, bundle.shape[1]),
        grid=(raw.shape[0],),
        out_shape=[jax.ShapeDtypeStruct(x.shape, x.dtype) for x in (raw, *smalls)],
        in_specs=[block, whole(bundle)] + [whole(x) for x in smalls],
        out_specs=[block] + [whole(x) for x in smalls],
        compiler_params=pltpu.CompilerParams(vmem_limit_bytes=40 * 1024 * 1024),
        cost_estimate=pl.CostEstimate(flops=0, bytes_accessed=2 * raw.size * raw.dtype.itemsize, transcendentals=0),
    )(raw, bundle, *smalls)


def fill_kernel(ns, pieces_ref, whole_ref, out_ref, sem):
    rows = pieces_ref.shape[1]
    z = lax.axis_index("shard")

    @pl.when((z == 0) | (z == ns - 1))
    def _():
        stores = []
        for slot in range(ns - 1):
            at = pl.multiple_of(shard_in(slot, ns) * rows, rows)
            spot = out_ref.at[out_ref.shape[0] - 1, pl.ds(at, rows), :]
            stores.append(pltpu.make_async_copy(pieces_ref.at[slot], spot, sem.at[slot]))
        for store in stores:
            store.start()
        for store in stores:
            store.wait()


def fill(ns, pieces, whole):
    anywhere = pl.BlockSpec(memory_space=pl.ANY)
    return pl.pallas_call(
        functools.partial(fill_kernel, ns),
        out_shape=jax.ShapeDtypeStruct(whole.shape, whole.dtype),
        in_specs=[pl.BlockSpec(memory_space=pltpu.VMEM), anywhere],
        out_specs=anywhere,
        input_output_aliases={1: 0},
        scratch_shapes=[pltpu.SemaphoreType.DMA((ns - 1,))],
        compiler_params=pltpu.CompilerParams(vmem_limit_bytes=32 * 1024 * 1024),
    )(pieces, whole)


def solution(mesh):
    ns, ne = mesh.shape["shard"], mesh.shape["expert"]
    assert ns >= 4

    def per_device(w_gate, avg_gate, w_up, avg_up, mix_share, router_weight, router_gain):
        experts, rows, cols = w_gate.shape
        n = 2 * experts
        ahead = max(cols // HEAD_PARTS // 128, 1) * 128
        dma = pltpu.SemaphoreType.DMA
        f32, bf16 = jnp.float32, jnp.bfloat16
        anywhere = pl.BlockSpec(memory_space=pl.ANY)
        serve = jax.ShapeDtypeStruct((experts, ns * rows, cols), bf16)
        scale = jax.ShapeDtypeStruct((experts, cols), f32)
        bundle = jax.ShapeDtypeStruct((ns - 1, rows, cols), bf16)
        table = jax.ShapeDtypeStruct((ne, ns, experts, rows), bf16)
        raw_gate, raw_up, scale_gate, scale_up, bundle, table = pl.pallas_call(
            functools.partial(kernel, ns, ne, experts, rows, cols, ahead),
            out_shape=(serve, serve, scale, scale, bundle, table),
            in_specs=[anywhere] * 7,
            out_specs=(anywhere,) * 6,
            scratch_shapes=[
                pltpu.VMEM((n, rows, cols), f32),
                pltpu.VMEM((SLOTS, rows, cols), f32),
                pltpu.VMEM((n, rows, cols), bf16),
                pltpu.VMEM((ns, 1, ahead), f32),
                pltpu.VMEM((ns, 2, cols), f32),
                pltpu.VMEM((ns, max(n - 2, 1), cols), f32),
                pltpu.VMEM((2, experts, cols), f32),
                pltpu.SMEM((experts,), f32),
                pltpu.VMEM((experts, rows), f32),
                pltpu.VMEM((1, rows), f32),
                pltpu.VMEM((ns, experts, rows), bf16),
                dma((n,)),
                dma((SLOTS,)),
                dma((2,)),
                dma((3,)),
                dma((n,)),
                dma((ns, n)),
                dma((ns - 1, n)),
                dma((ns - 1, n)),
                dma((ns,)),
                dma((ns,)),
                dma((ns,)),
                dma((ns,)),
                dma((ns,)),
                dma((ns,)),
                dma((ns,)),
                dma((ns,)),
                dma((ne,)),
                dma((ne,)),
                dma((3,)),
            ],
            compiler_params=pltpu.CompilerParams(
                collective_id=0, has_side_effects=True, vmem_limit_bytes=62 * 1024 * 1024
            ),
        )(mix_share, w_gate, avg_gate, w_up, avg_up, router_weight.T, router_gain.reshape(1, rows))
        pieces = lax.ppermute(bundle, "shard", [(1, 0), (ns - 2, ns - 1)])
        serve_gate = move(raw_gate)
        whole, scale_gate, scale_up, table = move_all(ns, raw_up, bundle, (scale_gate, scale_up, table))
        serve_up = fill(ns, pieces, whole)
        serve_router = table.transpose(1, 3, 0, 2).reshape(ns * rows, ne * experts)
        return serve_gate, serve_up, scale_gate, scale_up, serve_router

    return jax.shard_map(
        per_device,
        mesh=mesh,
        in_specs=(
            P("expert", "shard", None),
            P("expert", "shard", None),
            P("expert", "shard", None),
            P("expert", "shard", None),
            P("expert"),
            P("shard", "expert"),
            P("shard"),
        ),
        out_specs=(
            P("expert", None, None),
            P("expert", None, None),
            P("expert", None),
            P("expert", None),
            P(),
        ),
        check_vma=False,
    )
```

```python
import functools

import jax
import jax.numpy as jnp
from jax import lax
from jax.experimental import pallas as pl
from jax.experimental.pallas import tpu as pltpu
from jax.sharding import PartitionSpec as P

MESH = pl.DeviceIdType.MESH
SLOTS = 4
ROWS = 16
HEAD_PARTS = 4


def kernel(
    ns, ne, experts, rows, cols, ahead,
    mix_ref, wg_ref, ag_ref, wu_ref, au_ref, router_ref, gain_ref,
    og_ref, ou_ref, sg_ref, su_ref, bundle_ref, table_ref,
    fresh, other, narrow, first_sums, head, tail, scale, mix_s, weight, gain, column,
    load_sem, first_sem, small_sem, local_sem, recv_sem, last_recv, send_sem, last_send,
    sums_sem, column_sem, table_sem, own_sem,
):
    z, me = lax.axis_index("shard"), lax.axis_index("expert")
    n = 2 * experts
    half = ns // 2
    firsts, seconds, outs = (wg_ref, wu_ref), (ag_ref, au_ref), (og_ref, ou_ref)
    lead, follow = pl.ds(0, ahead), pl.ds(ahead, cols - ahead)
    inner = (z > 0) & (z < ns - 1)
    outer = jnp.logical_not(inner)

    def load_part(part, sem):
        pltpu.make_async_copy(wg_ref.at[0, :, part], fresh.at[0, :, part], sem).start()
        pltpu.make_async_copy(ag_ref.at[0, :, part], other.at[0, :, part], sem).start()

    def wait_for(ref, sem):
        pltpu.make_async_copy(ref, ref, sem).wait()

    get_mix = pltpu.make_async_copy(mix_ref, mix_s, small_sem.at[0])
    get_weight = pltpu.make_async_copy(router_ref, weight, small_sem.at[1])
    get_gain = pltpu.make_async_copy(gain_ref, gain, small_sem.at[2])

    load_part(lead, first_sem.at[0])
    get_mix.start()

    barrier = pltpu.get_barrier_semaphore()
    for k in range(1, ns):
        pl.semaphore_signal(barrier, inc=1, device_id={"shard": lax.rem(z + k, ns)}, device_id_type=MESH)

    def greet(k, carry):
        pl.semaphore_signal(barrier, inc=1, device_id={"expert": lax.rem(me + k, ne)}, device_id_type=MESH)
        return carry

    lax.fori_loop(1, ne, greet, 0)
    get_weight.start()
    get_gain.start()

    def slot_of(e, which):
        return lax.rem(2 * e + which, SLOTS)

    def load(e, which):
        c, slot = 2 * e + which, slot_of(e, which)
        pltpu.make_async_copy(firsts[which].at[e], fresh.at[c], load_sem.at[slot]).start()
        pltpu.make_async_copy(seconds[which].at[e], other.at[slot], load_sem.at[slot]).start()

    def loaded(e, which):
        wait_for(fresh.at[pl.ds(0, 2)], load_sem.at[slot_of(e, which)])

    def refill(e, which):
        @pl.when(e + SLOTS // 2 < experts)
        def _():
            load(e + SLOTS // 2, which)

    def place(e, which, j):
        return outs[which].at[e, pl.ds(pl.multiple_of(j * rows, rows), rows), :]

    def local_copy(e, which):
        return pltpu.make_async_copy(narrow.at[2 * e + which], place(e, which, z), local_sem.at[0])

    def hop(src, dst, step, send, recv):
        return pltpu.make_async_remote_copy(
            src_ref=src, dst_ref=dst, send_sem=send, recv_sem=recv,
            device_id={"shard": z + step}, device_id_type=MESH,
        )

    def sent(step, d):
        return send_sem.at[0 if step > 0 else 1, d]

    def send_on(e, which, step, d):
        j = z - step * d
        spot = place(e, which, j)
        src = narrow.at[2 * e + which] if d == 0 else spot
        hop(src, spot, step, sent(step, d), recv_sem.at[j, e]).start()

    def send_part(part, step):
        hop(narrow.at[0, :, part], place(0, 0, z).at[:, part], step, sent(step, 0), recv_sem.at[z, 0]).start()

    def pieces(count):
        return narrow.at[pl.ds(0, count)]

    def plain_at(device, j):
        return jnp.where(device < half, j == 0, j == ns - 1)

    def slot_at(device, j):
        return jnp.where(device < half, j - 1, j)

    def last_sent(step, d):
        return last_send.at[0 if step > 0 else 1, d]

    def last_goes(step, d):
        j = z - step * d
        return (z + step >= 1) & (z + step <= ns - 2) & (j >= 0) & (j <= ns - 1)

    def send_last(step, d):
        j = z - step * d
        goes, here, there = last_goes(step, d), plain_at(z, j), plain_at(z + step, j)
        spot = place(experts - 1, 1, j)
        for from_plain in (False, True):
            if d == 0 and from_plain:
                continue
            for to_plain in (False, True):
                fits = goes & (there if to_plain else jnp.logical_not(there))
                if d > 0:
                    fits = fits & (here if from_plain else jnp.logical_not(here))

                @pl.when(fits)
                def _():
                    src = narrow.at[n - 1] if d == 0 else spot if from_plain else bundle_ref.at[slot_at(z, j)]
                    dst = spot if to_plain else bundle_ref.at[slot_at(z + step, j)]
                    hop(src, dst, step, last_sent(step, d), last_recv.at[j]).start()

    def block_of(part, device, group, send, recv, slot):
        return pltpu.make_async_remote_copy(
            src_ref=part.at[slot], dst_ref=part.at[slot], send_sem=sums_sem.at[group, send],
            recv_sem=sums_sem.at[group, recv], device_id={"shard": device}, device_id_type=MESH,
        )

    def exchange(part, group):
        for device in range(1, ns - 1):
            pl.when(z != device)(lambda: block_of(part, device, group, 0, 1, z).start())

    def collect(part, group):
        @pl.when(inner)
        def _():
            wait_for(part.at[pl.ds(0, ns - 1)], sums_sem.at[group, 1])
            total = part[0]
            for j in range(1, ns):
                total = total + part[j]
            part[ns] = total

        @pl.when(outer)
        def _():
            wait_for(part.at[ns], sums_sem.at[group, 3])

    def tell(part, group):
        for device, end in ((1, 0), (ns - 2, ns - 1)):
            pl.when(z == device)(lambda: block_of(part, end, group, 2, 3, ns).start())

    def exchanged(part, group):
        pl.when(inner)(lambda: wait_for(part.at[pl.ds(0, ns - 3)], sums_sem.at[group, 0]))
        pl.when(outer)(lambda: wait_for(part.at[pl.ds(0, ns - 2)], sums_sem.at[group, 0]))
        pl.when((z == 1) | (z == ns - 2))(lambda: wait_for(part.at[ns], sums_sem.at[group, 2]))

    def send_column(k):
        pltpu.make_async_remote_copy(
            src_ref=column.at[z], dst_ref=column.at[z], send_sem=column_sem.at[0], recv_sem=column_sem.at[1],
            device_id={"shard": lax.rem(z + k, ns)}, device_id_type=MESH,
        ).start()

    def send_table(k, carry):
        pltpu.make_async_remote_copy(
            src_ref=column, dst_ref=table_ref.at[me], send_sem=table_sem.at[0], recv_sem=table_sem.at[1],
            device_id={"expert": lax.rem(me + k, ne)}, device_id_type=MESH,
        ).start()
        return carry

    own_table = pltpu.make_async_copy(column, table_ref.at[me], own_sem.at[0])

    def mix(c, e, slot, part, row, lo=0, hi=cols, height=ROWS):
        span = pl.ds(lo, hi - lo)
        share = mix_s[e]
        rest = 1.0 - share

        def step(i, acc):
            r = pl.ds(pl.multiple_of(i * height, height), height)
            value = share * fresh[c, r, span] + rest * other[slot, r, span]
            fresh[c, r, span] = value
            square = value * value
            for k in range(0, height, 8):
                acc = acc + square[k : k + 8]
            return acc

        acc = lax.fori_loop(0, rows // height, step, jnp.zeros((8, hi - lo), jnp.float32), unroll=2)
        part[z, pl.ds(row, 1), span] = jnp.sum(acc, axis=0, keepdims=True)

    def divide(c, e, which, part, row, lo=0, hi=cols, height=ROWS):
        span = pl.ds(lo, hi - lo)
        root = jnp.sqrt(part[ns, pl.ds(row, 1), span])
        scale[which, pl.ds(e, 1), span] = root
        wide = jnp.broadcast_to(root, (8, hi - lo))
        wide = jnp.concatenate([wide] * (height // 8), axis=0)

        def step(i, carry):
            r = pl.ds(pl.multiple_of(i * height, height), height)
            narrow[c, r, span] = (fresh[c, r, span] / wide).astype(jnp.bfloat16)
            return carry

        lax.fori_loop(0, rows // height, step, 0, unroll=2)

    def both_ways(go):
        pl.when(z > 0)(lambda: go(-1))
        pl.when(z < ns - 1)(lambda: go(1))

    def finish(e, which, part, row):
        divide(2 * e + which, e, which, part, row)

        def send():
            both_ways(lambda step: send_on(e, which, step, 0))
            local_copy(e, which).start()

        if which == 0:
            send()
        else:
            pl.when(e < experts - 1)(send)

    get_mix.wait()
    wait_for(fresh.at[pl.ds(0, 2), :, lead], first_sem.at[0])
    load_part(follow, load_sem.at[0])
    load(0, 1)
    mix(0, 0, 0, first_sums, 0, 0, ahead, 4 * ROWS)
    pl.semaphore_wait(barrier, ns - 1 + ne - 1)
    exchange(first_sums, 0)
    get_weight.wait()
    get_gain.wait()
    column[z] = (weight[...] * gain[...]).astype(jnp.bfloat16)
    wait_for(fresh.at[pl.ds(0, 2), :, follow], load_sem.at[0])
    if experts > 1:
        load(1, 0)
        load(1, 1)
    mix(0, 0, 0, head, 0, ahead, cols)
    refill(0, 0)
    for k in range(1, ns):
        send_column(k)
    loaded(0, 1)
    mix(1, 0, 1, head, 1)
    refill(0, 1)
    exchange(head, 1)
    collect(first_sums, 0)
    divide(0, 0, 0, first_sums, 0, 0, ahead, 4 * ROWS)
    tell(first_sums, 0)
    both_ways(lambda step: send_part(lead, step))
    if experts > 1:
        loaded(1, 0)
        mix(2, 1, 2, tail, 0)
        refill(1, 0)
    collect(head, 1)
    divide(0, 0, 0, head, 0, ahead, cols)
    both_ways(lambda step: send_part(follow, step))
    tell(head, 1)
    local_copy(0, 0).start()
    if experts > 1:
        loaded(1, 1)
        mix(3, 1, 3, tail, 1)
        refill(1, 1)

        def more(e, carry):
            for which in range(2):
                loaded(e, which)
                mix(2 * e + which, e, slot_of(e, which), tail, 2 * (e - 1) + which)
                refill(e, which)
            return carry

        lax.fori_loop(2, experts, more, 0)
        exchange(tail, 2)
    finish(0, 1, head, 1)
    if experts > 1:
        collect(tail, 2)
        finish(1, 0, tail, 0)
        tell(tail, 2)
        finish(1, 1, tail, 1)

        def rest(e, carry):
            for which in range(2):
                finish(e, which, tail, 2 * (e - 1) + which)
            return carry

        lax.fori_loop(2, experts, rest, 0)

    for step in (-1, 1):
        send_last(step, 0)

    @pl.when(inner)
    def _():
        pltpu.make_async_copy(narrow.at[n - 1], bundle_ref.at[slot_at(z, z)], local_sem.at[0]).start()

    @pl.when(outer)
    def _():
        local_copy(experts - 1, 1).start()

    for which, ref in enumerate((sg_ref, su_ref)):
        pltpu.make_async_copy(scale.at[which], ref, own_sem.at[1]).start()

    wait_for(column.at[pl.ds(0, ns - 1)], column_sem.at[1])
    own_table.start()
    lax.fori_loop(1, ne, send_table, 0)

    def each(step):
        def one(e, carry):
            step(e, 2)
            return carry

        lax.fori_loop(0, experts - 1, one, 0)
        step(experts - 1, 1)

    def land(e, count, d):
        pl.when(z >= d)(lambda: wait_for(pieces(count), recv_sem.at[z - d, e]))
        pl.when(z + d < ns)(lambda: wait_for(pieces(count), recv_sem.at[z + d, e]))

    def goes_on(step, d):
        return (z + d < ns) & (z > 0) if step < 0 else (z >= d) & (z < ns - 1)

    for d in range(1, ns - 1):
        def pass_on(e, count, d=d):
            land(e, count, d)
            for step in (-1, 1):
                @pl.when(goes_on(step, d))
                def _():
                    for which in range(count):
                        send_on(e, which, step, d)

        each(pass_on)

        @pl.when(inner)
        def _():
            pl.when(z >= d)(lambda: wait_for(pieces(1), last_recv.at[z - d]))
            pl.when(z + d < ns)(lambda: wait_for(pieces(1), last_recv.at[z + d]))

        for step in (-1, 1):
            send_last(step, d)

    wait_for(pieces(n), local_sem.at[0])
    wait_for(scale, own_sem.at[1])
    own_table.wait()
    for i in range(2):
        wait_for(table_ref.at[pl.ds(0, ne - 1)], table_sem.at[i])
    wait_for(column.at[pl.ds(0, ns - 1)], column_sem.at[0])
    for group, part in enumerate((first_sums, head, tail)[: 3 if experts > 1 else 2]):
        exchanged(part, group)
    for d in range(ns - 1):
        for step in (-1, 1):
            pl.when(last_goes(step, d))(lambda: wait_for(pieces(1), last_sent(step, d)))
    for d in range(ns - 1):
        for step in (-1, 1):
            pl.when(goes_on(step, d))(lambda: wait_for(pieces(n - 1), sent(step, d)))
    each(lambda e, count: land(e, count, ns - 1))


def shard_in(slot, ns):
    z = lax.axis_index("shard")
    return jnp.where(z < ns // 2, slot + 1, slot)


def move_kernel(src_ref, dst_ref):
    dst_ref[...] = src_ref[...]


def move(raw):
    block = pl.BlockSpec((1,) + raw.shape[1:], lambda i: (i, 0, 0))
    return pl.pallas_call(
        move_kernel,
        grid=(raw.shape[0],),
        out_shape=jax.ShapeDtypeStruct(raw.shape, raw.dtype),
        in_specs=[block],
        out_specs=block,
        compiler_params=pltpu.CompilerParams(vmem_limit_bytes=32 * 1024 * 1024),
        cost_estimate=pl.CostEstimate(flops=0, bytes_accessed=2 * raw.size * raw.dtype.itemsize, transcendentals=0),
    )(raw)


def move_all_kernel(ns, rows, raw_ref, bundle_ref, *refs):
    count = len(refs) // 2
    dst_ref, smalls, copies = refs[count], refs[:count], refs[count + 1 :]
    dst_ref[...] = raw_ref[...]
    z = lax.axis_index("shard")

    @pl.when(pl.program_id(0) == 0)
    def _():
        for small, copy in zip(smalls, copies):
            copy[...] = small[...]

    @pl.when((pl.program_id(0) == pl.num_programs(0) - 1) & (z > 0) & (z < ns - 1))
    def _():
        for slot in range(ns - 1):
            at = pl.multiple_of(shard_in(slot, ns) * rows, rows)
            dst_ref[0, pl.ds(at, rows), :] = bundle_ref[slot]


def move_all(ns, raw, bundle, smalls):
    block = pl.BlockSpec((1,) + raw.shape[1:], lambda i: (i, 0, 0))

    def whole(x):
        return pl.BlockSpec(x.shape, lambda i: (0,) * x.ndim)

    return pl.pallas_call(
        functools.partial(move_all_kernel, ns, bundle.shape[1]),
        grid=(raw.shape[0],),
        out_shape=[jax.ShapeDtypeStruct(x.shape, x.dtype) for x in (raw, *smalls)],
        in_specs=[block, whole(bundle)] + [whole(x) for x in smalls],
        out_specs=[block] + [whole(x) for x in smalls],
        compiler_params=pltpu.CompilerParams(vmem_limit_bytes=40 * 1024 * 1024),
        cost_estimate=pl.CostEstimate(flops=0, bytes_accessed=2 * raw.size * raw.dtype.itemsize, transcendentals=0),
    )(raw, bundle, *smalls)


def fill_kernel(ns, pieces_ref, whole_ref, out_ref, sem):
    rows = pieces_ref.shape[1]
    z = lax.axis_index("shard")

    @pl.when((z == 0) | (z == ns - 1))
    def _():
        stores = []
        for slot in range(ns - 1):
            at = pl.multiple_of(shard_in(slot, ns) * rows, rows)
            spot = out_ref.at[out_ref.shape[0] - 1, pl.ds(at, rows), :]
            stores.append(pltpu.make_async_copy(pieces_ref.at[slot], spot, sem.at[slot]))
        for store in stores:
            store.start()
        for store in stores:
            store.wait()


def fill(ns, pieces, whole):
    anywhere = pl.BlockSpec(memory_space=pl.ANY)
    return pl.pallas_call(
        functools.partial(fill_kernel, ns),
        out_shape=jax.ShapeDtypeStruct(whole.shape, whole.dtype),
        in_specs=[pl.BlockSpec(memory_space=pltpu.VMEM), anywhere],
        out_specs=anywhere,
        input_output_aliases={1: 0},
        scratch_shapes=[pltpu.SemaphoreType.DMA((ns - 1,))],
        compiler_params=pltpu.CompilerParams(vmem_limit_bytes=32 * 1024 * 1024),
    )(pieces, whole)


def solution(mesh):
    ns, ne = mesh.shape["shard"], mesh.shape["expert"]
    assert ns >= 4

    def per_device(w_gate, avg_gate, w_up, avg_up, mix_share, router_weight, router_gain):
        experts, rows, cols = w_gate.shape
        n = 2 * experts
        ahead = max(cols // HEAD_PARTS // 128, 1) * 128
        dma = pltpu.SemaphoreType.DMA
        f32, bf16 = jnp.float32, jnp.bfloat16
        anywhere = pl.BlockSpec(memory_space=pl.ANY)
        serve = jax.ShapeDtypeStruct((experts, ns * rows, cols), bf16)
        scale = jax.ShapeDtypeStruct((experts, cols), f32)
        bundle = jax.ShapeDtypeStruct((ns - 1, rows, cols), bf16)
        table = jax.ShapeDtypeStruct((ne, ns, experts, rows), bf16)
        raw_gate, raw_up, scale_gate, scale_up, bundle, table = pl.pallas_call(
            functools.partial(kernel, ns, ne, experts, rows, cols, ahead),
            out_shape=(serve, serve, scale, scale, bundle, table),
            in_specs=[anywhere] * 7,
            out_specs=(anywhere,) * 6,
            scratch_shapes=[
                pltpu.VMEM((n, rows, cols), f32),
                pltpu.VMEM((SLOTS, rows, cols), f32),
                pltpu.VMEM((n, rows, cols), bf16),
                pltpu.VMEM((ns + 1, 1, ahead), f32),
                pltpu.VMEM((ns + 1, 2, cols), f32),
                pltpu.VMEM((ns + 1, max(n - 2, 1), cols), f32),
                pltpu.VMEM((2, experts, cols), f32),
                pltpu.SMEM((experts,), f32),
                pltpu.VMEM((experts, rows), f32),
                pltpu.VMEM((1, rows), f32),
                pltpu.VMEM((ns, experts, rows), bf16),
                dma((SLOTS,)),
                dma((1,)),
                dma((3,)),
                dma((1,)),
                dma((ns, experts)),
                dma((ns,)),
                dma((2, ns - 1)),
                dma((2, ns - 1)),
                dma((3, 4)),
                dma((2,)),
                dma((2,)),
                dma((2,)),
            ],
            compiler_params=pltpu.CompilerParams(
                collective_id=0, has_side_effects=True, vmem_limit_bytes=62 * 1024 * 1024
            ),
        )(mix_share, w_gate, avg_gate, w_up, avg_up, router_weight.T, router_gain.reshape(1, rows))
        pieces = lax.ppermute(bundle, "shard", [(1, 0), (ns - 2, ns - 1)])
        serve_gate = move(raw_gate)
        whole, scale_gate, scale_up, table = move_all(ns, raw_up, bundle, (scale_gate, scale_up, table))
        serve_up = fill(ns, pieces, whole)
        serve_router = table.transpose(1, 3, 0, 2).reshape(ns * rows, ne * experts)
        return serve_gate, serve_up, scale_gate, scale_up, serve_router

    return jax.shard_map(
        per_device,
        mesh=mesh,
        in_specs=(
            P("expert", "shard", None),
            P("expert", "shard", None),
            P("expert", "shard", None),
            P("expert", "shard", None),
            P("expert"),
            P("shard", "expert"),
            P("shard"),
        ),
        out_specs=(
            P("expert", None, None),
            P("expert", None, None),
            P("expert", None),
            P("expert", None),
            P(),
        ),
        check_vma=False,
    )
```

```python
import functools

import jax
import jax.numpy as jnp
from jax import lax
from jax.experimental import pallas as pl
from jax.experimental.pallas import tpu as pltpu
from jax.sharding import PartitionSpec as P

MESH = pl.DeviceIdType.MESH
SLOTS = 4
ROWS = 16
HEAD_PARTS = 4
EDGE = 128


def kernel(
    ns, ne, experts, rows, cols, ahead, top, splits,
    mix_ref, wg_ref, ag_ref, wu_ref, au_ref, router_ref, gain_ref,
    og_ref, ou_ref, sg_ref, su_ref, big_ref, small_ref, table_ref,
    fresh, other, narrow, first_sums, head, tail, scale, mix_s, weight, gain, column, edge32, edge16,
    load_sem, first_sem, small_sem, local_sem, recv_sem, last_recv, send_sem, last_send,
    sums_sem, column_sem, table_sem, own_sem, edge_sem,
):
    z, me = lax.axis_index("shard"), lax.axis_index("expert")
    n = 2 * experts
    half = ns // 2
    firsts, seconds, outs = (wg_ref, wu_ref), (ag_ref, au_ref), (og_ref, ou_ref)
    lead, follow = pl.ds(0, ahead), pl.ds(ahead, cols - ahead)
    inner = (z > 0) & (z < ns - 1)
    outer = jnp.logical_not(inner)
    near = jnp.where(z == 0, 1, ns - 2)
    edge_rows = rows - top * EDGE // cols
    bundles = tuple(zip((big_ref, small_ref), splits))

    def outward(step):
        return z == 1 if step < 0 else z == ns - 2

    def load_part(part, sem):
        pltpu.make_async_copy(wg_ref.at[0, :, part], fresh.at[0, :, part], sem).start()
        pltpu.make_async_copy(ag_ref.at[0, :, part], other.at[0, :, part], sem).start()

    def wait_for(ref, sem):
        pltpu.make_async_copy(ref, ref, sem).wait()

    get_mix = pltpu.make_async_copy(mix_ref, mix_s, small_sem.at[0])
    get_weight = pltpu.make_async_copy(router_ref, weight, small_sem.at[1])
    get_gain = pltpu.make_async_copy(gain_ref, gain, small_sem.at[2])

    load_part(lead, first_sem.at[0])
    get_mix.start()

    barrier = pltpu.get_barrier_semaphore()
    for k in range(1, ns):
        pl.semaphore_signal(barrier, inc=1, device_id={"shard": lax.rem(z + k, ns)}, device_id_type=MESH)

    def greet(k, carry):
        pl.semaphore_signal(barrier, inc=1, device_id={"expert": lax.rem(me + k, ne)}, device_id_type=MESH)
        return carry

    lax.fori_loop(1, ne, greet, 0)
    get_weight.start()
    get_gain.start()

    def slot_of(e, which):
        return lax.rem(2 * e + which, SLOTS)

    def load(e, which):
        c, slot = 2 * e + which, slot_of(e, which)
        pltpu.make_async_copy(firsts[which].at[e], fresh.at[c], load_sem.at[slot]).start()
        pltpu.make_async_copy(seconds[which].at[e], other.at[slot], load_sem.at[slot]).start()

    def loaded(e, which):
        wait_for(fresh.at[pl.ds(0, 2)], load_sem.at[slot_of(e, which)])

    def refill(e, which):
        @pl.when(e + SLOTS // 2 < experts)
        def _():
            load(e + SLOTS // 2, which)

    def place(e, which, j):
        return outs[which].at[e, pl.ds(pl.multiple_of(j * rows, rows), rows), :]

    def local_copy(e, which):
        return pltpu.make_async_copy(narrow.at[2 * e + which], place(e, which, z), local_sem.at[0])

    def hop(src, dst, step, send, recv):
        return pltpu.make_async_remote_copy(
            src_ref=src, dst_ref=dst, send_sem=send, recv_sem=recv,
            device_id={"shard": z + step}, device_id_type=MESH,
        )

    def sent(step, d):
        return send_sem.at[0 if step > 0 else 1, d]

    def send_on(e, which, step, d):
        j = z - step * d
        spot = place(e, which, j)
        src = narrow.at[2 * e + which] if d == 0 else spot
        hop(src, spot, step, sent(step, d), recv_sem.at[j, e]).start()

    def send_block(r, c, step, send):
        hop(narrow.at[0, r, c], place(0, 0, z).at[r, c], step, send, recv_sem.at[z, 0]).start()

    def send_edge(step):
        @pl.when(outward(step))
        def _():
            hop(fresh.at[0, pl.ds(0, top), pl.ds(0, EDGE)], edge32, step, edge_sem.at[0], edge_sem.at[1]).start()

    def send_lead(step):
        @pl.when(outward(step))
        def _():
            if ahead > EDGE:
                send_block(pl.ds(0, rows), pl.ds(EDGE, ahead - EDGE), step, edge_sem.at[2])
            send_block(pl.ds(top, rows - top), pl.ds(0, EDGE), step, edge_sem.at[2])

        @pl.when(jnp.logical_not(outward(step)))
        def _():
            send_block(pl.ds(0, rows), lead, step, sent(step, 0))

    def send_follow(step):
        @pl.when(outward(step))
        def _():
            send_block(pl.ds(0, rows), follow, step, edge_sem.at[2])

        @pl.when(jnp.logical_not(outward(step)))
        def _():
            send_block(pl.ds(0, rows), follow, step, sent(step, 0))

    def divide_edge():
        wait_for(edge32, edge_sem.at[1])
        wide = jnp.broadcast_to(scale[0, pl.ds(0, 1), pl.ds(0, EDGE)], (8, EDGE))
        wide = jnp.concatenate([wide] * (ROWS // 8), axis=0)

        def step(i, carry):
            r = pl.ds(pl.multiple_of(i * ROWS, ROWS), ROWS)
            edge16[r, :] = (edge32[r, :] / wide).astype(jnp.bfloat16)
            return carry

        lax.fori_loop(0, top // ROWS, step, 0)

    def pieces(count):
        return narrow.at[pl.ds(0, count)]

    def plain_at(device, j):
        return jnp.where(device < half, j == 0, j == ns - 1)

    def slot_at(device, j):
        return jnp.where(device < half, j - 1, j)

    def last_sent(step, d):
        return last_send.at[0 if step > 0 else 1, d]

    def last_goes(step, d):
        j = z - step * d
        return (z + step >= 1) & (z + step <= ns - 2) & (j >= 0) & (j <= ns - 1)

    def send_last(step, d):
        j = z - step * d
        goes, here, there = last_goes(step, d), plain_at(z, j), plain_at(z + step, j)
        spot = place(experts - 1, 1, j)
        for from_plain in (False, True):
            if d == 0 and from_plain:
                continue
            for to_plain in (False, True):
                fits = goes & (there if to_plain else jnp.logical_not(there))
                if d > 0:
                    fits = fits & (here if from_plain else jnp.logical_not(here))

                @pl.when(fits)
                def _():
                    for ref, (lo, size) in bundles:
                        part = pl.ds(lo, size)
                        plain = spot.at[part]
                        src = narrow.at[n - 1, part] if d == 0 else plain if from_plain else ref.at[slot_at(z, j)]
                        dst = plain if to_plain else ref.at[slot_at(z + step, j)]
                        hop(src, dst, step, last_sent(step, d), last_recv.at[j]).start()

    def block_of(part, device, group, send, recv, slot):
        return pltpu.make_async_remote_copy(
            src_ref=part.at[slot], dst_ref=part.at[slot], send_sem=sums_sem.at[group, send],
            recv_sem=sums_sem.at[group, recv], device_id={"shard": device}, device_id_type=MESH,
        )

    def exchange(part, group):
        for device in range(1, ns - 1):
            pl.when(z != device)(lambda: block_of(part, device, group, 0, 1, z).start())

    def collect(part, group):
        @pl.when(inner)
        def _():
            wait_for(part.at[pl.ds(0, ns - 1)], sums_sem.at[group, 1])
            total = part[0]
            for j in range(1, ns):
                total = total + part[j]
            part[ns] = total

        @pl.when(outer)
        def _():
            wait_for(part.at[ns], sums_sem.at[group, 3])

    def tell(part, group):
        for device, end in ((1, 0), (ns - 2, ns - 1)):
            pl.when(z == device)(lambda: block_of(part, end, group, 2, 3, ns).start())

    def exchanged(part, group):
        pl.when(inner)(lambda: wait_for(part.at[pl.ds(0, ns - 3)], sums_sem.at[group, 0]))
        pl.when(outer)(lambda: wait_for(part.at[pl.ds(0, ns - 2)], sums_sem.at[group, 0]))
        pl.when((z == 1) | (z == ns - 2))(lambda: wait_for(part.at[ns], sums_sem.at[group, 2]))

    def send_column(k):
        pltpu.make_async_remote_copy(
            src_ref=column.at[z], dst_ref=column.at[z], send_sem=column_sem.at[0], recv_sem=column_sem.at[1],
            device_id={"shard": lax.rem(z + k, ns)}, device_id_type=MESH,
        ).start()

    def send_table(k, carry):
        pltpu.make_async_remote_copy(
            src_ref=column, dst_ref=table_ref.at[me], send_sem=table_sem.at[0], recv_sem=table_sem.at[1],
            device_id={"expert": lax.rem(me + k, ne)}, device_id_type=MESH,
        ).start()
        return carry

    own_table = pltpu.make_async_copy(column, table_ref.at[me], own_sem.at[0])

    def mix(c, e, slot, part, row, lo=0, hi=cols, height=ROWS):
        span = pl.ds(lo, hi - lo)
        share = mix_s[e]
        rest = 1.0 - share

        def step(i, acc):
            r = pl.ds(pl.multiple_of(i * height, height), height)
            value = share * fresh[c, r, span] + rest * other[slot, r, span]
            fresh[c, r, span] = value
            square = value * value
            for k in range(0, height, 8):
                acc = acc + square[k : k + 8]
            return acc

        acc = lax.fori_loop(0, rows // height, step, jnp.zeros((8, hi - lo), jnp.float32), unroll=2)
        part[z, pl.ds(row, 1), span] = jnp.sum(acc, axis=0, keepdims=True)

    def divide(c, e, which, part, row, lo=0, hi=cols, height=ROWS):
        span = pl.ds(lo, hi - lo)
        root = jnp.sqrt(part[ns, pl.ds(row, 1), span])
        scale[which, pl.ds(e, 1), span] = root
        wide = jnp.broadcast_to(root, (8, hi - lo))
        wide = jnp.concatenate([wide] * (height // 8), axis=0)

        def step(i, carry):
            r = pl.ds(pl.multiple_of(i * height, height), height)
            narrow[c, r, span] = (fresh[c, r, span] / wide).astype(jnp.bfloat16)
            return carry

        lax.fori_loop(0, rows // height, step, 0, unroll=2)

    def both_ways(go):
        pl.when(z > 0)(lambda: go(-1))
        pl.when(z < ns - 1)(lambda: go(1))

    def finish(e, which, part, row):
        divide(2 * e + which, e, which, part, row)

        def send():
            both_ways(lambda step: send_on(e, which, step, 0))
            local_copy(e, which).start()

        if which == 0:
            send()
        else:
            pl.when(e < experts - 1)(send)

    get_mix.wait()
    wait_for(fresh.at[pl.ds(0, 2), :, lead], first_sem.at[0])
    load_part(follow, load_sem.at[0])
    load(0, 1)
    mix(0, 0, 0, first_sums, 0, 0, ahead, 4 * ROWS)
    pl.semaphore_wait(barrier, ns - 1 + ne - 1)
    exchange(first_sums, 0)
    for step in (-1, 1):
        send_edge(step)
    get_weight.wait()
    get_gain.wait()
    column[z] = (weight[...] * gain[...]).astype(jnp.bfloat16)
    wait_for(fresh.at[pl.ds(0, 2), :, follow], load_sem.at[0])
    if experts > 1:
        load(1, 0)
        load(1, 1)
    mix(0, 0, 0, head, 0, ahead, cols)
    refill(0, 0)
    for k in range(1, ns):
        send_column(k)
    loaded(0, 1)
    mix(1, 0, 1, head, 1)
    refill(0, 1)
    exchange(head, 1)
    collect(first_sums, 0)
    divide(0, 0, 0, first_sums, 0, 0, ahead, 4 * ROWS)
    tell(first_sums, 0)
    both_ways(send_lead)
    if experts > 1:
        loaded(1, 0)
        mix(2, 1, 2, tail, 0)
        refill(1, 0)
    collect(head, 1)
    divide(0, 0, 0, head, 0, ahead, cols)
    both_ways(send_follow)
    tell(head, 1)
    local_copy(0, 0).start()
    if experts > 1:
        loaded(1, 1)
        mix(3, 1, 3, tail, 1)
        refill(1, 1)

        def more(e, carry):
            for which in range(2):
                loaded(e, which)
                mix(2 * e + which, e, slot_of(e, which), tail, 2 * (e - 1) + which)
                refill(e, which)
            return carry

        lax.fori_loop(2, experts, more, 0)
        exchange(tail, 2)
    finish(0, 1, head, 1)
    if experts > 1:
        collect(tail, 2)
        finish(1, 0, tail, 0)
        tell(tail, 2)
        finish(1, 1, tail, 1)

        def rest(e, carry):
            for which in range(2):
                finish(e, which, tail, 2 * (e - 1) + which)
            return carry

        lax.fori_loop(2, experts, rest, 0)

    for step in (-1, 1):
        send_last(step, 0)

    @pl.when(inner)
    def _():
        for ref, (lo, size) in bundles:
            own = narrow.at[n - 1, pl.ds(lo, size)]
            pltpu.make_async_copy(own, ref.at[slot_at(z, z)], local_sem.at[0]).start()

    @pl.when(outer)
    def _():
        local_copy(experts - 1, 1).start()
        divide_edge()

    for which, ref in enumerate((sg_ref, su_ref)):
        pltpu.make_async_copy(scale.at[which], ref, own_sem.at[1]).start()

    wait_for(column.at[pl.ds(0, ns - 1)], column_sem.at[1])
    own_table.start()
    lax.fori_loop(1, ne, send_table, 0)

    @pl.when(outer)
    def _():
        spot = place(0, 0, near).at[pl.ds(0, top), pl.ds(0, EDGE)]
        pltpu.make_async_copy(edge16, spot, edge_sem.at[3]).start()

    def each(step):
        def one(e, carry):
            step(e, 2)
            return carry

        if experts > 1:
            step(0, 2)
            lax.fori_loop(1, experts - 1, one, 0)
        step(experts - 1, 1)

    def land(e, count, d):
        for fits, j in ((z >= d, z - d), (z + d < ns, z + d)):
            if isinstance(e, int) and e == 0 and d == 1:
                short = og_ref.at[0, pl.ds(0, (count - 1) * rows + edge_rows), :]
                pl.when(fits & outer)(lambda: wait_for(short, recv_sem.at[j, 0]))
                fits = fits & inner
            pl.when(fits)(lambda: wait_for(pieces(count), recv_sem.at[j, e]))

    def goes_on(step, d):
        return (z + d < ns) & (z > 0) if step < 0 else (z >= d) & (z < ns - 1)

    for d in range(1, ns - 1):
        def pass_on(e, count, d=d):
            land(e, count, d)
            for step in (-1, 1):
                @pl.when(goes_on(step, d))
                def _():
                    for which in range(count):
                        send_on(e, which, step, d)

        each(pass_on)

        @pl.when(inner)
        def _():
            pl.when(z >= d)(lambda: wait_for(pieces(1), last_recv.at[z - d]))
            pl.when(z + d < ns)(lambda: wait_for(pieces(1), last_recv.at[z + d]))

        for step in (-1, 1):
            send_last(step, d)

    wait_for(pieces(n), local_sem.at[0])
    wait_for(scale, own_sem.at[1])
    own_table.wait()
    for i in range(2):
        wait_for(table_ref.at[pl.ds(0, ne - 1)], table_sem.at[i])
    wait_for(column.at[pl.ds(0, ns - 1)], column_sem.at[0])
    for group, part in enumerate((first_sums, head, tail)[: 3 if experts > 1 else 2]):
        exchanged(part, group)
    for d in range(ns - 1):
        for step in (-1, 1):
            pl.when(last_goes(step, d))(lambda: wait_for(pieces(1), last_sent(step, d)))
    @pl.when(outer)
    def _():
        wait_for(edge16, edge_sem.at[3])

    for d in range(ns - 1):
        for step in (-1, 1):
            fits = goes_on(step, d)
            if d == 0:
                @pl.when(outward(step))
                def _():
                    wait_for(edge32, edge_sem.at[0])
                    wait_for(narrow.at[0, pl.ds(0, edge_rows)], edge_sem.at[2])
                    if n > 2:
                        wait_for(pieces(n - 2), sent(step, 0))

                fits = fits & jnp.logical_not(outward(step))
            pl.when(fits)(lambda: wait_for(pieces(n - 1), sent(step, d)))
    each(lambda e, count: land(e, count, ns - 1))


def shard_in(slot, ns):
    z = lax.axis_index("shard")
    return jnp.where(z < ns // 2, slot + 1, slot)


def move_kernel(src_ref, dst_ref):
    dst_ref[...] = src_ref[...]


def move(raw):
    block = pl.BlockSpec((1,) + raw.shape[1:], lambda i: (i, 0, 0))
    return pl.pallas_call(
        move_kernel,
        grid=(raw.shape[0],),
        out_shape=jax.ShapeDtypeStruct(raw.shape, raw.dtype),
        in_specs=[block],
        out_specs=block,
        compiler_params=pltpu.CompilerParams(vmem_limit_bytes=32 * 1024 * 1024),
        cost_estimate=pl.CostEstimate(flops=0, bytes_accessed=2 * raw.size * raw.dtype.itemsize, transcendentals=0),
    )(raw)


def move_all_kernel(ns, rows, splits, raw_ref, big_ref, small_ref, *refs):
    count = len(refs) // 2
    dst_ref, smalls, copies = refs[count], refs[:count], refs[count + 1 :]
    dst_ref[...] = raw_ref[...]
    z = lax.axis_index("shard")

    @pl.when(pl.program_id(0) == 0)
    def _():
        for small, copy in zip(smalls, copies):
            copy[...] = small[...]

    @pl.when((pl.program_id(0) == pl.num_programs(0) - 1) & (z > 0) & (z < ns - 1))
    def _():
        for ref, (lo, size) in zip((big_ref, small_ref), splits):
            for slot in range(ns - 1):
                at = pl.multiple_of(shard_in(slot, ns) * rows + lo, 16)
                dst_ref[0, pl.ds(at, size), :] = ref[slot]


def move_all(ns, rows, splits, raw, bundles, smalls):
    block = pl.BlockSpec((1,) + raw.shape[1:], lambda i: (i, 0, 0))

    def whole(x):
        return pl.BlockSpec(x.shape, lambda i: (0,) * x.ndim)

    return pl.pallas_call(
        functools.partial(move_all_kernel, ns, rows, splits),
        grid=(raw.shape[0],),
        out_shape=[jax.ShapeDtypeStruct(x.shape, x.dtype) for x in (raw, *smalls)],
        in_specs=[block] + [whole(x) for x in (*bundles, *smalls)],
        out_specs=[block] + [whole(x) for x in smalls],
        compiler_params=pltpu.CompilerParams(vmem_limit_bytes=40 * 1024 * 1024),
        cost_estimate=pl.CostEstimate(flops=0, bytes_accessed=2 * raw.size * raw.dtype.itemsize, transcendentals=0),
    )(raw, *bundles, *smalls)


def fill_kernel(ns, rows, lo, pieces_ref, whole_ref, out_ref, sem):
    z = lax.axis_index("shard")

    @pl.when((z == 0) | (z == ns - 1))
    def _():
        stores = []
        for slot in range(ns - 1):
            at = pl.multiple_of(shard_in(slot, ns) * rows + lo, 16)
            spot = out_ref.at[out_ref.shape[0] - 1, pl.ds(at, pieces_ref.shape[1]), :]
            stores.append(pltpu.make_async_copy(pieces_ref.at[slot], spot, sem.at[slot]))
        for store in stores:
            store.start()
        for store in stores:
            store.wait()


def fill(ns, rows, lo, pieces, whole):
    anywhere = pl.BlockSpec(memory_space=pl.ANY)
    size = 2 * pieces.size * pieces.dtype.itemsize
    return pl.pallas_call(
        functools.partial(fill_kernel, ns, rows, lo),
        out_shape=jax.ShapeDtypeStruct(whole.shape, whole.dtype),
        in_specs=[pl.BlockSpec(memory_space=pltpu.VMEM), anywhere],
        out_specs=anywhere,
        input_output_aliases={1: 0},
        scratch_shapes=[pltpu.SemaphoreType.DMA((ns - 1,))],
        compiler_params=pltpu.CompilerParams(vmem_limit_bytes=32 * 1024 * 1024),
        cost_estimate=pl.CostEstimate(flops=0, bytes_accessed=size, transcendentals=0),
    )(pieces, whole)


def solution(mesh):
    ns, ne = mesh.shape["shard"], mesh.shape["expert"]
    assert ns >= 4

    def per_device(w_gate, avg_gate, w_up, avg_up, mix_share, router_weight, router_gain):
        experts, rows, cols = w_gate.shape
        n = 2 * experts
        ahead = max(cols // HEAD_PARTS // 128, 1) * 128
        top = rows * 3 // 4 // 16 * 16
        assert top * EDGE % cols == 0
        large = rows * 7 // 8 // 16 * 16
        splits = ((0, large), (large, rows - large))
        dma = pltpu.SemaphoreType.DMA
        f32, bf16 = jnp.float32, jnp.bfloat16
        anywhere = pl.BlockSpec(memory_space=pl.ANY)
        serve = jax.ShapeDtypeStruct((experts, ns * rows, cols), bf16)
        scale = jax.ShapeDtypeStruct((experts, cols), f32)
        bundles = tuple(jax.ShapeDtypeStruct((ns - 1, size, cols), bf16) for _, size in splits)
        table = jax.ShapeDtypeStruct((ne, ns, experts, rows), bf16)
        raw_gate, raw_up, scale_gate, scale_up, *bundles, table = pl.pallas_call(
            functools.partial(kernel, ns, ne, experts, rows, cols, ahead, top, splits),
            out_shape=(serve, serve, scale, scale, *bundles, table),
            in_specs=[anywhere] * 7,
            out_specs=(anywhere,) * 7,
            scratch_shapes=[
                pltpu.VMEM((n, rows, cols), f32),
                pltpu.VMEM((SLOTS, rows, cols), f32),
                pltpu.VMEM((n, rows, cols), bf16),
                pltpu.VMEM((ns + 1, 1, ahead), f32),
                pltpu.VMEM((ns + 1, 2, cols), f32),
                pltpu.VMEM((ns + 1, max(n - 2, 1), cols), f32),
                pltpu.VMEM((2, experts, cols), f32),
                pltpu.SMEM((experts,), f32),
                pltpu.VMEM((experts, rows), f32),
                pltpu.VMEM((1, rows), f32),
                pltpu.VMEM((ns, experts, rows), bf16),
                pltpu.VMEM((top, EDGE), f32),
                pltpu.VMEM((top, EDGE), bf16),
                dma((SLOTS,)),
                dma((1,)),
                dma((3,)),
                dma((1,)),
                dma((ns, experts)),
                dma((ns,)),
                dma((2, ns - 1)),
                dma((2, ns - 1)),
                dma((3, 4)),
                dma((2,)),
                dma((2,)),
                dma((2,)),
                dma((4,)),
            ],
            compiler_params=pltpu.CompilerParams(
                collective_id=0, has_side_effects=True, vmem_limit_bytes=62 * 1024 * 1024
            ),
        )(mix_share, w_gate, avg_gate, w_up, avg_up, router_weight.T, router_gain.reshape(1, rows))
        pieces = [lax.ppermute(bundle, "shard", [(1, 0), (ns - 2, ns - 1)]) for bundle in bundles]
        serve_gate = move(raw_gate)
        smalls = (scale_gate, scale_up, table)
        serve_up, scale_gate, scale_up, table = move_all(ns, rows, splits, raw_up, bundles, smalls)
        for (lo, _), piece in zip(splits, pieces):
            serve_up = fill(ns, rows, lo, piece, serve_up)
        serve_router = table.transpose(1, 3, 0, 2).reshape(ns * rows, ne * experts)
        return serve_gate, serve_up, scale_gate, scale_up, serve_router

    return jax.shard_map(
        per_device,
        mesh=mesh,
        in_specs=(
            P("expert", "shard", None),
            P("expert", "shard", None),
            P("expert", "shard", None),
            P("expert", "shard", None),
            P("expert"),
            P("shard", "expert"),
            P("shard"),
        ),
        out_specs=(
            P("expert", None, None),
            P("expert", None, None),
            P("expert", None),
            P("expert", None),
            P(),
        ),
        check_vma=False,
    )
```

```python
import functools

import jax
import jax.numpy as jnp
from jax import lax
from jax.experimental import pallas as pl
from jax.experimental.pallas import tpu as pltpu
from jax.sharding import PartitionSpec as P

MESH = pl.DeviceIdType.MESH
SLOTS = 4
ROWS = 16
HEAD_PARTS = 2
EDGE = 256


def kernel(
    ns, ne, experts, rows, cols, ahead, top, splits,
    mix_ref, wg_ref, ag_ref, wu_ref, au_ref, router_ref, gain_ref,
    og_ref, ou_ref, sg_ref, su_ref, big_ref, small_ref, table_ref,
    fresh, other, narrow, first_sums, head, tail, scale, mix_s, weight, gain, column, edge32, edge16,
    load_sem, first_sem, small_sem, local_sem, recv_sem, last_recv, send_sem, last_send,
    sums_sem, column_sem, table_sem, own_sem, edge_sem,
):
    z, me = lax.axis_index("shard"), lax.axis_index("expert")
    n = 2 * experts
    half = ns // 2
    firsts, seconds, outs = (wg_ref, wu_ref), (ag_ref, au_ref), (og_ref, ou_ref)
    lead, follow = pl.ds(0, ahead), pl.ds(ahead, cols - ahead)
    inner = (z > 0) & (z < ns - 1)
    outer = jnp.logical_not(inner)
    near = jnp.where(z == 0, 1, ns - 2)
    edge_rows = rows - top * EDGE // cols
    bundles = tuple(zip((big_ref, small_ref), splits))

    eager = lax.rem(me, 2) == 1
    edge_in = outer & eager

    def outward(step):
        return (z == 1 if step < 0 else z == ns - 2) & eager

    def load_part(part, sem):
        pltpu.make_async_copy(wg_ref.at[0, :, part], fresh.at[0, :, part], sem).start()
        pltpu.make_async_copy(ag_ref.at[0, :, part], other.at[0, :, part], sem).start()

    def wait_for(ref, sem):
        pltpu.make_async_copy(ref, ref, sem).wait()

    get_mix = pltpu.make_async_copy(mix_ref, mix_s, small_sem.at[0])
    get_weight = pltpu.make_async_copy(router_ref, weight, small_sem.at[1])
    get_gain = pltpu.make_async_copy(gain_ref, gain, small_sem.at[2])

    load_part(lead, first_sem.at[0])
    get_mix.start()

    barrier = pltpu.get_barrier_semaphore()
    for k in range(1, ns):
        pl.semaphore_signal(barrier, inc=1, device_id={"shard": lax.rem(z + k, ns)}, device_id_type=MESH)

    def greet(k, carry):
        pl.semaphore_signal(barrier, inc=1, device_id={"expert": lax.rem(me + k, ne)}, device_id_type=MESH)
        return carry

    lax.fori_loop(1, ne, greet, 0)
    get_weight.start()
    get_gain.start()

    def slot_of(e, which):
        return lax.rem(2 * e + which, SLOTS)

    def load(e, which):
        c, slot = 2 * e + which, slot_of(e, which)
        pltpu.make_async_copy(firsts[which].at[e], fresh.at[c], load_sem.at[slot]).start()
        pltpu.make_async_copy(seconds[which].at[e], other.at[slot], load_sem.at[slot]).start()

    def loaded(e, which):
        wait_for(fresh.at[pl.ds(0, 2)], load_sem.at[slot_of(e, which)])

    def refill(e, which):
        @pl.when(e + SLOTS // 2 < experts)
        def _():
            load(e + SLOTS // 2, which)

    def place(e, which, j):
        return outs[which].at[e, pl.ds(pl.multiple_of(j * rows, rows), rows), :]

    def local_copy(e, which):
        return pltpu.make_async_copy(narrow.at[2 * e + which], place(e, which, z), local_sem.at[0])

    def hop(src, dst, step, send, recv):
        return pltpu.make_async_remote_copy(
            src_ref=src, dst_ref=dst, send_sem=send, recv_sem=recv,
            device_id={"shard": z + step}, device_id_type=MESH,
        )

    def sent(step, d):
        return send_sem.at[0 if step > 0 else 1, d]

    def send_on(e, which, step, d):
        j = z - step * d
        spot = place(e, which, j)
        src = narrow.at[2 * e + which] if d == 0 else spot
        hop(src, spot, step, sent(step, d), recv_sem.at[j, e]).start()

    def send_block(r, c, step, send):
        hop(narrow.at[0, r, c], place(0, 0, z).at[r, c], step, send, recv_sem.at[z, 0]).start()

    def send_edge(step):
        @pl.when(outward(step))
        def _():
            hop(fresh.at[0, pl.ds(0, top), pl.ds(0, EDGE)], edge32, step, edge_sem.at[0], edge_sem.at[1]).start()

    def send_lead(step):
        @pl.when(outward(step))
        def _():
            if ahead > EDGE:
                send_block(pl.ds(0, rows), pl.ds(EDGE, ahead - EDGE), step, edge_sem.at[2])
            send_block(pl.ds(top, rows - top), pl.ds(0, EDGE), step, edge_sem.at[2])

        @pl.when(jnp.logical_not(outward(step)))
        def _():
            send_block(pl.ds(0, rows), lead, step, sent(step, 0))

    def send_follow(step):
        @pl.when(outward(step))
        def _():
            send_block(pl.ds(0, rows), follow, step, edge_sem.at[2])

        @pl.when(jnp.logical_not(outward(step)))
        def _():
            send_block(pl.ds(0, rows), follow, step, sent(step, 0))

    def divide_edge():
        wait_for(edge32, edge_sem.at[1])
        wide = jnp.broadcast_to(scale[0, pl.ds(0, 1), pl.ds(0, EDGE)], (8, EDGE))
        wide = jnp.concatenate([wide] * (ROWS // 8), axis=0)

        def step(i, carry):
            r = pl.ds(pl.multiple_of(i * ROWS, ROWS), ROWS)
            edge16[r, :] = (edge32[r, :] / wide).astype(jnp.bfloat16)
            return carry

        lax.fori_loop(0, top // ROWS, step, 0)

    def pieces(count):
        return narrow.at[pl.ds(0, count)]

    def plain_at(device, j):
        return jnp.where(device < half, j == 0, j == ns - 1)

    def slot_at(device, j):
        return jnp.where(device < half, j - 1, j)

    def last_sent(step, d):
        return last_send.at[0 if step > 0 else 1, d]

    def last_goes(step, d):
        j = z - step * d
        return (z + step >= 1) & (z + step <= ns - 2) & (j >= 0) & (j <= ns - 1)

    def send_last(step, d):
        j = z - step * d
        goes, here, there = last_goes(step, d), plain_at(z, j), plain_at(z + step, j)
        spot = place(experts - 1, 1, j)
        for from_plain in (False, True):
            if d == 0 and from_plain:
                continue
            for to_plain in (False, True):
                fits = goes & (there if to_plain else jnp.logical_not(there))
                if d > 0:
                    fits = fits & (here if from_plain else jnp.logical_not(here))

                @pl.when(fits)
                def _():
                    for ref, (lo, size) in bundles:
                        part = pl.ds(lo, size)
                        plain = spot.at[part]
                        src = narrow.at[n - 1, part] if d == 0 else plain if from_plain else ref.at[slot_at(z, j)]
                        dst = plain if to_plain else ref.at[slot_at(z + step, j)]
                        hop(src, dst, step, last_sent(step, d), last_recv.at[j]).start()

    def block_of(part, device, group, send, recv, slot):
        return pltpu.make_async_remote_copy(
            src_ref=part.at[slot], dst_ref=part.at[slot], send_sem=sums_sem.at[group, send],
            recv_sem=sums_sem.at[group, recv], device_id={"shard": device}, device_id_type=MESH,
        )

    def exchange(part, group):
        for device in range(1, ns - 1):
            pl.when(z != device)(lambda: block_of(part, device, group, 0, 1, z).start())

    def collect(part, group):
        @pl.when(inner)
        def _():
            wait_for(part.at[pl.ds(0, ns - 1)], sums_sem.at[group, 1])
            total = part[0]
            for j in range(1, ns):
                total = total + part[j]
            part[ns] = total

        @pl.when(outer)
        def _():
            wait_for(part.at[ns], sums_sem.at[group, 3])

    def tell(part, group):
        for device, end in ((1, 0), (ns - 2, ns - 1)):
            pl.when(z == device)(lambda: block_of(part, end, group, 2, 3, ns).start())

    def exchanged(part, group):
        pl.when(inner)(lambda: wait_for(part.at[pl.ds(0, ns - 3)], sums_sem.at[group, 0]))
        pl.when(outer)(lambda: wait_for(part.at[pl.ds(0, ns - 2)], sums_sem.at[group, 0]))
        pl.when((z == 1) | (z == ns - 2))(lambda: wait_for(part.at[ns], sums_sem.at[group, 2]))

    def send_column(k):
        pltpu.make_async_remote_copy(
            src_ref=column.at[z], dst_ref=column.at[z], send_sem=column_sem.at[0], recv_sem=column_sem.at[1],
            device_id={"shard": lax.rem(z + k, ns)}, device_id_type=MESH,
        ).start()

    def send_table(k, carry):
        pltpu.make_async_remote_copy(
            src_ref=column, dst_ref=table_ref.at[me], send_sem=table_sem.at[0], recv_sem=table_sem.at[1],
            device_id={"expert": lax.rem(me + k, ne)}, device_id_type=MESH,
        ).start()
        return carry

    own_table = pltpu.make_async_copy(column, table_ref.at[me], own_sem.at[0])

    def mix(c, e, slot, part, row, lo=0, hi=cols, height=ROWS):
        span = pl.ds(lo, hi - lo)
        share = mix_s[e]
        rest = 1.0 - share

        def step(i, acc):
            r = pl.ds(pl.multiple_of(i * height, height), height)
            value = share * fresh[c, r, span] + rest * other[slot, r, span]
            fresh[c, r, span] = value
            square = value * value
            for k in range(0, height, 8):
                acc = acc + square[k : k + 8]
            return acc

        acc = lax.fori_loop(0, rows // height, step, jnp.zeros((8, hi - lo), jnp.float32), unroll=2)
        part[z, pl.ds(row, 1), span] = jnp.sum(acc, axis=0, keepdims=True)

    def divide(c, e, which, part, row, lo=0, hi=cols, height=ROWS):
        span = pl.ds(lo, hi - lo)
        root = jnp.sqrt(part[ns, pl.ds(row, 1), span])
        scale[which, pl.ds(e, 1), span] = root
        wide = jnp.broadcast_to(root, (8, hi - lo))
        wide = jnp.concatenate([wide] * (height // 8), axis=0)

        def step(i, carry):
            r = pl.ds(pl.multiple_of(i * height, height), height)
            narrow[c, r, span] = (fresh[c, r, span] / wide).astype(jnp.bfloat16)
            return carry

        lax.fori_loop(0, rows // height, step, 0, unroll=2)

    def both_ways(go):
        pl.when(z > 0)(lambda: go(-1))
        pl.when(z < ns - 1)(lambda: go(1))

    def finish(e, which, part, row):
        divide(2 * e + which, e, which, part, row)

        def send():
            both_ways(lambda step: send_on(e, which, step, 0))
            local_copy(e, which).start()

        if which == 0:
            send()
        else:
            pl.when(e < experts - 1)(send)

    get_mix.wait()
    wait_for(fresh.at[pl.ds(0, 2), :, lead], first_sem.at[0])
    load_part(follow, load_sem.at[0])
    load(0, 1)
    mix(0, 0, 0, first_sums, 0, 0, ahead, 4 * ROWS)
    pl.semaphore_wait(barrier, ns - 1 + ne - 1)
    exchange(first_sums, 0)
    for step in (-1, 1):
        send_edge(step)
    get_weight.wait()
    get_gain.wait()
    column[z] = (weight[...] * gain[...]).astype(jnp.bfloat16)
    wait_for(fresh.at[pl.ds(0, 2), :, follow], load_sem.at[0])
    if experts > 1:
        load(1, 0)
        load(1, 1)
    mix(0, 0, 0, head, 0, ahead, cols)
    refill(0, 0)
    for k in range(1, ns):
        send_column(k)
    loaded(0, 1)
    mix(1, 0, 1, head, 1)
    refill(0, 1)
    exchange(head, 1)
    collect(first_sums, 0)
    divide(0, 0, 0, first_sums, 0, 0, ahead, 4 * ROWS)
    tell(first_sums, 0)
    pl.when(eager)(lambda: both_ways(send_lead))
    if experts > 1:
        loaded(1, 0)
        mix(2, 1, 2, tail, 0)
        refill(1, 0)
    collect(head, 1)
    divide(0, 0, 0, head, 0, ahead, cols)
    pl.when(jnp.logical_not(eager))(lambda: both_ways(send_lead))
    both_ways(send_follow)
    tell(head, 1)
    local_copy(0, 0).start()
    if experts > 1:
        loaded(1, 1)
        mix(3, 1, 3, tail, 1)
        refill(1, 1)

        def more(e, carry):
            for which in range(2):
                loaded(e, which)
                mix(2 * e + which, e, slot_of(e, which), tail, 2 * (e - 1) + which)
                refill(e, which)
            return carry

        lax.fori_loop(2, experts, more, 0)
        exchange(tail, 2)
    finish(0, 1, head, 1)
    if experts > 1:
        collect(tail, 2)
        finish(1, 0, tail, 0)
        tell(tail, 2)
        finish(1, 1, tail, 1)

        def rest(e, carry):
            for which in range(2):
                finish(e, which, tail, 2 * (e - 1) + which)
            return carry

        lax.fori_loop(2, experts, rest, 0)

    for step in (-1, 1):
        send_last(step, 0)

    @pl.when(inner)
    def _():
        for ref, (lo, size) in bundles:
            own = narrow.at[n - 1, pl.ds(lo, size)]
            pltpu.make_async_copy(own, ref.at[slot_at(z, z)], local_sem.at[0]).start()

    @pl.when(outer)
    def _():
        local_copy(experts - 1, 1).start()

    pl.when(edge_in)(divide_edge)

    for which, ref in enumerate((sg_ref, su_ref)):
        pltpu.make_async_copy(scale.at[which], ref, own_sem.at[1]).start()

    wait_for(column.at[pl.ds(0, ns - 1)], column_sem.at[1])
    own_table.start()
    lax.fori_loop(1, ne, send_table, 0)

    @pl.when(edge_in)
    def _():
        spot = place(0, 0, near).at[pl.ds(0, top), pl.ds(0, EDGE)]
        pltpu.make_async_copy(edge16, spot, edge_sem.at[3]).start()

    def each(step):
        def one(e, carry):
            step(e, 2)
            return carry

        if experts > 1:
            step(0, 2)
            lax.fori_loop(1, experts - 1, one, 0)
        step(experts - 1, 1)

    def land(e, count, d):
        for fits, j in ((z >= d, z - d), (z + d < ns, z + d)):
            if isinstance(e, int) and e == 0 and d == 1:
                short = og_ref.at[0, pl.ds(0, (count - 1) * rows + edge_rows), :]
                pl.when(fits & edge_in)(lambda: wait_for(short, recv_sem.at[j, 0]))
                fits = fits & jnp.logical_not(edge_in)
            pl.when(fits)(lambda: wait_for(pieces(count), recv_sem.at[j, e]))

    def goes_on(step, d):
        return (z + d < ns) & (z > 0) if step < 0 else (z >= d) & (z < ns - 1)

    for d in range(1, ns - 1):
        def pass_on(e, count, d=d):
            land(e, count, d)
            for step in (-1, 1):
                @pl.when(goes_on(step, d))
                def _():
                    for which in range(count):
                        send_on(e, which, step, d)

        each(pass_on)

        @pl.when(inner)
        def _():
            pl.when(z >= d)(lambda: wait_for(pieces(1), last_recv.at[z - d]))
            pl.when(z + d < ns)(lambda: wait_for(pieces(1), last_recv.at[z + d]))

        for step in (-1, 1):
            send_last(step, d)

    wait_for(pieces(n), local_sem.at[0])
    wait_for(scale, own_sem.at[1])
    own_table.wait()
    for i in range(2):
        wait_for(table_ref.at[pl.ds(0, ne - 1)], table_sem.at[i])
    wait_for(column.at[pl.ds(0, ns - 1)], column_sem.at[0])
    for group, part in enumerate((first_sums, head, tail)[: 3 if experts > 1 else 2]):
        exchanged(part, group)
    for d in range(ns - 1):
        for step in (-1, 1):
            pl.when(last_goes(step, d))(lambda: wait_for(pieces(1), last_sent(step, d)))
    @pl.when(edge_in)
    def _():
        wait_for(edge16, edge_sem.at[3])

    for d in range(ns - 1):
        for step in (-1, 1):
            fits = goes_on(step, d)
            if d == 0:
                @pl.when(outward(step))
                def _():
                    wait_for(edge32, edge_sem.at[0])
                    wait_for(narrow.at[0, pl.ds(0, edge_rows)], edge_sem.at[2])
                    if n > 2:
                        wait_for(pieces(n - 2), sent(step, 0))

                fits = fits & jnp.logical_not(outward(step))
            pl.when(fits)(lambda: wait_for(pieces(n - 1), sent(step, d)))
    each(lambda e, count: land(e, count, ns - 1))


def shard_in(slot, ns):
    z = lax.axis_index("shard")
    return jnp.where(z < ns // 2, slot + 1, slot)


def move_kernel(src_ref, dst_ref):
    dst_ref[...] = src_ref[...]


def move(raw):
    block = pl.BlockSpec((1,) + raw.shape[1:], lambda i: (i, 0, 0))
    return pl.pallas_call(
        move_kernel,
        grid=(raw.shape[0],),
        out_shape=jax.ShapeDtypeStruct(raw.shape, raw.dtype),
        in_specs=[block],
        out_specs=block,
        compiler_params=pltpu.CompilerParams(vmem_limit_bytes=32 * 1024 * 1024),
        cost_estimate=pl.CostEstimate(flops=0, bytes_accessed=2 * raw.size * raw.dtype.itemsize, transcendentals=0),
    )(raw)


def move_all_kernel(ns, rows, splits, raw_ref, big_ref, small_ref, *refs):
    count = len(refs) // 2
    dst_ref, smalls, copies = refs[count], refs[:count], refs[count + 1 :]
    dst_ref[...] = raw_ref[...]
    z = lax.axis_index("shard")

    @pl.when(pl.program_id(0) == 0)
    def _():
        for small, copy in zip(smalls, copies):
            copy[...] = small[...]

    @pl.when((pl.program_id(0) == pl.num_programs(0) - 1) & (z > 0) & (z < ns - 1))
    def _():
        for ref, (lo, size) in zip((big_ref, small_ref), splits):
            for slot in range(ns - 1):
                at = pl.multiple_of(shard_in(slot, ns) * rows + lo, 16)
                dst_ref[0, pl.ds(at, size), :] = ref[slot]


def move_all(ns, rows, splits, raw, bundles, smalls):
    block = pl.BlockSpec((1,) + raw.shape[1:], lambda i: (i, 0, 0))

    def whole(x):
        return pl.BlockSpec(x.shape, lambda i: (0,) * x.ndim)

    return pl.pallas_call(
        functools.partial(move_all_kernel, ns, rows, splits),
        grid=(raw.shape[0],),
        out_shape=[jax.ShapeDtypeStruct(x.shape, x.dtype) for x in (raw, *smalls)],
        in_specs=[block] + [whole(x) for x in (*bundles, *smalls)],
        out_specs=[block] + [whole(x) for x in smalls],
        compiler_params=pltpu.CompilerParams(vmem_limit_bytes=40 * 1024 * 1024),
        cost_estimate=pl.CostEstimate(flops=0, bytes_accessed=2 * raw.size * raw.dtype.itemsize, transcendentals=0),
    )(raw, *bundles, *smalls)


def fill_kernel(ns, rows, lo, pieces_ref, whole_ref, out_ref, sem):
    z = lax.axis_index("shard")

    @pl.when((z == 0) | (z == ns - 1))
    def _():
        stores = []
        for slot in range(ns - 1):
            at = pl.multiple_of(shard_in(slot, ns) * rows + lo, 16)
            spot = out_ref.at[out_ref.shape[0] - 1, pl.ds(at, pieces_ref.shape[1]), :]
            stores.append(pltpu.make_async_copy(pieces_ref.at[slot], spot, sem.at[slot]))
        for store in stores:
            store.start()
        for store in stores:
            store.wait()


def fill(ns, rows, lo, pieces, whole):
    anywhere = pl.BlockSpec(memory_space=pl.ANY)
    size = 2 * pieces.size * pieces.dtype.itemsize
    return pl.pallas_call(
        functools.partial(fill_kernel, ns, rows, lo),
        out_shape=jax.ShapeDtypeStruct(whole.shape, whole.dtype),
        in_specs=[pl.BlockSpec(memory_space=pltpu.VMEM), anywhere],
        out_specs=anywhere,
        input_output_aliases={1: 0},
        scratch_shapes=[pltpu.SemaphoreType.DMA((ns - 1,))],
        compiler_params=pltpu.CompilerParams(vmem_limit_bytes=32 * 1024 * 1024),
        cost_estimate=pl.CostEstimate(flops=0, bytes_accessed=size, transcendentals=0),
    )(pieces, whole)


def solution(mesh):
    ns, ne = mesh.shape["shard"], mesh.shape["expert"]
    assert ns >= 4

    def per_device(w_gate, avg_gate, w_up, avg_up, mix_share, router_weight, router_gain):
        experts, rows, cols = w_gate.shape
        n = 2 * experts
        ahead = max(cols // HEAD_PARTS // 128, 1) * 128
        top = rows * 3 // 4 // 16 * 16
        assert top * EDGE % cols == 0
        large = rows * 7 // 8 // 16 * 16
        splits = ((0, large), (large, rows - large))
        dma = pltpu.SemaphoreType.DMA
        f32, bf16 = jnp.float32, jnp.bfloat16
        anywhere = pl.BlockSpec(memory_space=pl.ANY)
        serve = jax.ShapeDtypeStruct((experts, ns * rows, cols), bf16)
        scale = jax.ShapeDtypeStruct((experts, cols), f32)
        bundles = tuple(jax.ShapeDtypeStruct((ns - 1, size, cols), bf16) for _, size in splits)
        table = jax.ShapeDtypeStruct((ne, ns, experts, rows), bf16)
        raw_gate, raw_up, scale_gate, scale_up, *bundles, table = pl.pallas_call(
            functools.partial(kernel, ns, ne, experts, rows, cols, ahead, top, splits),
            out_shape=(serve, serve, scale, scale, *bundles, table),
            in_specs=[anywhere] * 7,
            out_specs=(anywhere,) * 7,
            scratch_shapes=[
                pltpu.VMEM((n, rows, cols), f32),
                pltpu.VMEM((SLOTS, rows, cols), f32),
                pltpu.VMEM((n, rows, cols), bf16),
                pltpu.VMEM((ns + 1, 1, ahead), f32),
                pltpu.VMEM((ns + 1, 2, cols), f32),
                pltpu.VMEM((ns + 1, max(n - 2, 1), cols), f32),
                pltpu.VMEM((2, experts, cols), f32),
                pltpu.SMEM((experts,), f32),
                pltpu.VMEM((experts, rows), f32),
                pltpu.VMEM((1, rows), f32),
                pltpu.VMEM((ns, experts, rows), bf16),
                pltpu.VMEM((top, EDGE), f32),
                pltpu.VMEM((top, EDGE), bf16),
                dma((SLOTS,)),
                dma((1,)),
                dma((3,)),
                dma((1,)),
                dma((ns, experts)),
                dma((ns,)),
                dma((2, ns - 1)),
                dma((2, ns - 1)),
                dma((3, 4)),
                dma((2,)),
                dma((2,)),
                dma((2,)),
                dma((4,)),
            ],
            compiler_params=pltpu.CompilerParams(
                collective_id=0, has_side_effects=True, vmem_limit_bytes=62 * 1024 * 1024
            ),
        )(mix_share, w_gate, avg_gate, w_up, avg_up, router_weight.T, router_gain.reshape(1, rows))
        pieces = [lax.ppermute(bundle, "shard", [(1, 0), (ns - 2, ns - 1)]) for bundle in bundles]
        serve_gate = move(raw_gate)
        smalls = (scale_gate, scale_up, table)
        serve_up, scale_gate, scale_up, table = move_all(ns, rows, splits, raw_up, bundles, smalls)
        for (lo, _), piece in zip(splits, pieces):
            serve_up = fill(ns, rows, lo, piece, serve_up)
        serve_router = table.transpose(1, 3, 0, 2).reshape(ns * rows, ne * experts)
        return serve_gate, serve_up, scale_gate, scale_up, serve_router

    return jax.shard_map(
        per_device,
        mesh=mesh,
        in_specs=(
            P("expert", "shard", None),
            P("expert", "shard", None),
            P("expert", "shard", None),
            P("expert", "shard", None),
            P("expert"),
            P("shard", "expert"),
            P("shard"),
        ),
        out_specs=(
            P("expert", None, None),
            P("expert", None, None),
            P("expert", None),
            P("expert", None),
            P(),
        ),
        check_vma=False,
    )
```

```python
import functools

import jax
import jax.numpy as jnp
from jax import lax
from jax.experimental import pallas as pl
from jax.experimental.pallas import tpu as pltpu
from jax.sharding import PartitionSpec as P

MESH = pl.DeviceIdType.MESH
SLOTS = 4
ROWS = 16
HEAD_PARTS = 2
EDGE = 256


def kernel(
    ns, ne, experts, rows, cols, ahead, top, splits,
    mix_ref, wg_ref, ag_ref, wu_ref, au_ref, router_ref, gain_ref,
    og_ref, ou_ref, sg_ref, su_ref, big_ref, small_ref, table_ref,
    fresh, other, narrow, first_sums, head, tail, scale, mix_s, weight, gain, column, edge32, edge16,
    load_sem, first_sem, small_sem, local_sem, recv_sem, last_recv, send_sem, last_send,
    sums_sem, column_sem, table_sem, own_sem, edge_sem,
):
    z, me = lax.axis_index("shard"), lax.axis_index("expert")
    n = 2 * experts
    half = ns // 2
    firsts, seconds, outs = (wg_ref, wu_ref), (ag_ref, au_ref), (og_ref, ou_ref)
    lead, follow = pl.ds(0, ahead), pl.ds(ahead, cols - ahead)
    inner = (z > 0) & (z < ns - 1)
    outer = jnp.logical_not(inner)
    near = jnp.where(z == 0, 1, ns - 2)
    edge_rows = rows - top * EDGE // cols
    bundles = tuple(zip((big_ref, small_ref), splits))

    eager = lax.rem(me, 2) == 1
    edge_in = outer & eager

    def outward(step):
        return (z == 1 if step < 0 else z == ns - 2) & eager

    def load_part(part, sem):
        pltpu.make_async_copy(wg_ref.at[0, :, part], fresh.at[0, :, part], sem).start()
        pltpu.make_async_copy(ag_ref.at[0, :, part], other.at[0, :, part], sem).start()

    def wait_for(ref, sem):
        pltpu.make_async_copy(ref, ref, sem).wait()

    get_mix = pltpu.make_async_copy(mix_ref, mix_s, small_sem.at[0])
    get_weight = pltpu.make_async_copy(router_ref, weight, small_sem.at[1])
    get_gain = pltpu.make_async_copy(gain_ref, gain, small_sem.at[2])

    load_part(lead, first_sem.at[0])
    get_mix.start()

    barrier = pltpu.get_barrier_semaphore()
    for k in range(1, ns):
        pl.semaphore_signal(barrier, inc=1, device_id={"shard": lax.rem(z + k, ns)}, device_id_type=MESH)

    def greet(k, carry):
        pl.semaphore_signal(barrier, inc=1, device_id={"expert": lax.rem(me + k, ne)}, device_id_type=MESH)
        return carry

    lax.fori_loop(1, ne, greet, 0)
    get_weight.start()
    get_gain.start()

    def slot_of(e, which):
        return lax.rem(2 * e + which, SLOTS)

    def load(e, which):
        c, slot = 2 * e + which, slot_of(e, which)
        pltpu.make_async_copy(firsts[which].at[e], fresh.at[c], load_sem.at[slot]).start()
        pltpu.make_async_copy(seconds[which].at[e], other.at[slot], load_sem.at[slot]).start()

    def loaded(e, which):
        wait_for(fresh.at[pl.ds(0, 2)], load_sem.at[slot_of(e, which)])

    def refill(e, which):
        @pl.when(e + SLOTS // 2 < experts)
        def _():
            load(e + SLOTS // 2, which)

    def place(e, which, j):
        return outs[which].at[e, pl.ds(pl.multiple_of(j * rows, rows), rows), :]

    def local_copy(e, which):
        return pltpu.make_async_copy(narrow.at[2 * e + which], place(e, which, z), local_sem.at[0])

    def hop(src, dst, step, send, recv):
        return pltpu.make_async_remote_copy(
            src_ref=src, dst_ref=dst, send_sem=send, recv_sem=recv,
            device_id={"shard": z + step}, device_id_type=MESH,
        )

    def sent(step, d):
        return send_sem.at[0 if step > 0 else 1, d]

    def send_on(e, which, step, d):
        j = z - step * d
        spot = place(e, which, j)
        src = narrow.at[2 * e + which] if d == 0 else spot
        hop(src, spot, step, sent(step, d), recv_sem.at[j, e]).start()

    def send_block(r, c, step, send):
        hop(narrow.at[0, r, c], place(0, 0, z).at[r, c], step, send, recv_sem.at[z, 0]).start()

    def send_edge(step):
        @pl.when(outward(step))
        def _():
            hop(fresh.at[0, pl.ds(0, top), pl.ds(0, EDGE)], edge32, step, edge_sem.at[0], edge_sem.at[1]).start()

    def send_lead(step):
        @pl.when(outward(step))
        def _():
            if ahead > EDGE:
                send_block(pl.ds(0, rows), pl.ds(EDGE, ahead - EDGE), step, edge_sem.at[2])
            send_block(pl.ds(top, rows - top), pl.ds(0, EDGE), step, edge_sem.at[2])

        @pl.when(jnp.logical_not(outward(step)))
        def _():
            send_block(pl.ds(0, rows), lead, step, sent(step, 0))

    def send_follow(step):
        @pl.when(outward(step))
        def _():
            send_block(pl.ds(0, rows), follow, step, edge_sem.at[2])

        @pl.when(jnp.logical_not(outward(step)))
        def _():
            send_block(pl.ds(0, rows), follow, step, sent(step, 0))

    def divide_edge():
        wait_for(edge32, edge_sem.at[1])
        wide = jnp.broadcast_to(scale[0, pl.ds(0, 1), pl.ds(0, EDGE)], (8, EDGE))
        wide = jnp.concatenate([wide] * (ROWS // 8), axis=0)

        def step(i, carry):
            r = pl.ds(pl.multiple_of(i * ROWS, ROWS), ROWS)
            edge16[r, :] = (edge32[r, :] / wide).astype(jnp.bfloat16)
            return carry

        lax.fori_loop(0, top // ROWS, step, 0)

    def pieces(count):
        return narrow.at[pl.ds(0, count)]

    def plain_at(device, j):
        return jnp.where(device < half, j == 0, j == ns - 1)

    def slot_at(device, j):
        return jnp.where(device < half, j - 1, j)

    def last_sent(step, d):
        return last_send.at[0 if step > 0 else 1, d]

    def last_goes(step, d):
        j = z - step * d
        return (z + step >= 1) & (z + step <= ns - 2) & (j >= 0) & (j <= ns - 1)

    def send_last(step, d):
        j = z - step * d
        goes, here, there = last_goes(step, d), plain_at(z, j), plain_at(z + step, j)
        spot = place(experts - 1, 1, j)
        for from_plain in (False, True):
            if d == 0 and from_plain:
                continue
            for to_plain in (False, True):
                fits = goes & (there if to_plain else jnp.logical_not(there))
                if d > 0:
                    fits = fits & (here if from_plain else jnp.logical_not(here))

                @pl.when(fits)
                def _():
                    for ref, (lo, size) in bundles:
                        part = pl.ds(lo, size)
                        plain = spot.at[part]
                        src = narrow.at[n - 1, part] if d == 0 else plain if from_plain else ref.at[slot_at(z, j)]
                        dst = plain if to_plain else ref.at[slot_at(z + step, j)]
                        hop(src, dst, step, last_sent(step, d), last_recv.at[j]).start()

    def block_of(part, device, group, send, recv, slot):
        return pltpu.make_async_remote_copy(
            src_ref=part.at[slot], dst_ref=part.at[slot], send_sem=sums_sem.at[group, send],
            recv_sem=sums_sem.at[group, recv], device_id={"shard": device}, device_id_type=MESH,
        )

    def exchange(part, group):
        for device in range(1, ns - 1):
            pl.when(z != device)(lambda: block_of(part, device, group, 0, 1, z).start())

    def collect(part, group):
        @pl.when(inner)
        def _():
            wait_for(part.at[pl.ds(0, ns - 1)], sums_sem.at[group, 1])
            total = part[0]
            for j in range(1, ns):
                total = total + part[j]
            part[ns] = total

        @pl.when(outer)
        def _():
            wait_for(part.at[ns], sums_sem.at[group, 3])

    def tell(part, group):
        for device, end in ((1, 0), (ns - 2, ns - 1)):
            pl.when(z == device)(lambda: block_of(part, end, group, 2, 3, ns).start())

    def exchanged(part, group):
        pl.when(inner)(lambda: wait_for(part.at[pl.ds(0, ns - 3)], sums_sem.at[group, 0]))
        pl.when(outer)(lambda: wait_for(part.at[pl.ds(0, ns - 2)], sums_sem.at[group, 0]))
        pl.when((z == 1) | (z == ns - 2))(lambda: wait_for(part.at[ns], sums_sem.at[group, 2]))

    def send_column(k):
        pltpu.make_async_remote_copy(
            src_ref=column.at[z], dst_ref=column.at[z], send_sem=column_sem.at[0], recv_sem=column_sem.at[1],
            device_id={"shard": lax.rem(z + k, ns)}, device_id_type=MESH,
        ).start()

    def send_table(k, carry):
        pltpu.make_async_remote_copy(
            src_ref=column, dst_ref=table_ref.at[me], send_sem=table_sem.at[0], recv_sem=table_sem.at[1],
            device_id={"expert": lax.rem(me + k, ne)}, device_id_type=MESH,
        ).start()
        return carry

    own_table = pltpu.make_async_copy(column, table_ref.at[me], own_sem.at[0])

    def mix(c, e, slot, part, row, lo=0, hi=cols, height=ROWS):
        span = pl.ds(lo, hi - lo)
        share = mix_s[e]
        rest = 1.0 - share

        def step(i, acc):
            r = pl.ds(pl.multiple_of(i * height, height), height)
            value = share * fresh[c, r, span] + rest * other[slot, r, span]
            fresh[c, r, span] = value
            square = value * value
            for k in range(0, height, 8):
                acc = acc + square[k : k + 8]
            return acc

        acc = lax.fori_loop(0, rows // height, step, jnp.zeros((8, hi - lo), jnp.float32), unroll=2)
        part[z, pl.ds(row, 1), span] = jnp.sum(acc, axis=0, keepdims=True)

    def divide(c, e, which, part, row, lo=0, hi=cols, height=ROWS):
        span = pl.ds(lo, hi - lo)
        root = jnp.sqrt(part[ns, pl.ds(row, 1), span])
        scale[which, pl.ds(e, 1), span] = root
        wide = jnp.broadcast_to(root, (8, hi - lo))
        wide = jnp.concatenate([wide] * (height // 8), axis=0)

        def step(i, carry):
            r = pl.ds(pl.multiple_of(i * height, height), height)
            narrow[c, r, span] = (fresh[c, r, span] / wide).astype(jnp.bfloat16)
            return carry

        lax.fori_loop(0, rows // height, step, 0, unroll=2)

    def both_ways(go):
        pl.when(z > 0)(lambda: go(-1))
        pl.when(z < ns - 1)(lambda: go(1))

    def finish(e, which, part, row):
        divide(2 * e + which, e, which, part, row)

        def send():
            both_ways(lambda step: send_on(e, which, step, 0))
            local_copy(e, which).start()

        if which == 0:
            send()
        else:
            pl.when(e < experts - 1)(send)

    get_mix.wait()
    wait_for(fresh.at[pl.ds(0, 2), :, lead], first_sem.at[0])
    load_part(follow, load_sem.at[0])
    load(0, 1)
    mix(0, 0, 0, first_sums, 0, 0, ahead, 4 * ROWS)
    pl.semaphore_wait(barrier, ns - 1 + ne - 1)
    exchange(first_sums, 0)
    for step in (-1, 1):
        send_edge(step)
    get_weight.wait()
    get_gain.wait()
    column[z] = (weight[...] * gain[...]).astype(jnp.bfloat16)
    wait_for(fresh.at[pl.ds(0, 2), :, follow], load_sem.at[0])
    if experts > 1:
        load(1, 0)
        load(1, 1)
    mix(0, 0, 0, head, 0, ahead, cols)
    refill(0, 0)
    for k in range(1, ns):
        send_column(k)
    loaded(0, 1)
    mix(1, 0, 1, head, 1)
    refill(0, 1)
    exchange(head, 1)
    collect(first_sums, 0)
    divide(0, 0, 0, first_sums, 0, 0, ahead, 4 * ROWS)
    tell(first_sums, 0)
    pl.when(eager)(lambda: both_ways(send_lead))
    if experts > 1:
        loaded(1, 0)
        mix(2, 1, 2, tail, 0)
        refill(1, 0)
    collect(head, 1)
    divide(0, 0, 0, head, 0, ahead, cols)
    pl.when(jnp.logical_not(eager))(lambda: both_ways(send_lead))
    both_ways(send_follow)
    tell(head, 1)
    local_copy(0, 0).start()
    if experts > 1:
        loaded(1, 1)
        mix(3, 1, 3, tail, 1)
        refill(1, 1)

        def more(e, carry):
            for which in range(2):
                loaded(e, which)
                mix(2 * e + which, e, slot_of(e, which), tail, 2 * (e - 1) + which)
                refill(e, which)
            return carry

        lax.fori_loop(2, experts, more, 0)
        exchange(tail, 2)
    finish(0, 1, head, 1)
    if experts > 1:
        collect(tail, 2)
        finish(1, 0, tail, 0)
        tell(tail, 2)
        finish(1, 1, tail, 1)

        def rest(e, carry):
            for which in range(2):
                finish(e, which, tail, 2 * (e - 1) + which)
            return carry

        lax.fori_loop(2, experts, rest, 0)

    for step in (-1, 1):
        send_last(step, 0)

    @pl.when(inner)
    def _():
        for ref, (lo, size) in bundles:
            own = narrow.at[n - 1, pl.ds(lo, size)]
            pltpu.make_async_copy(own, ref.at[slot_at(z, z)], local_sem.at[0]).start()

    @pl.when(outer)
    def _():
        local_copy(experts - 1, 1).start()

    pl.when(edge_in)(divide_edge)

    for which, ref in enumerate((sg_ref, su_ref)):
        pltpu.make_async_copy(scale.at[which], ref, own_sem.at[1]).start()

    wait_for(column.at[pl.ds(0, ns - 1)], column_sem.at[1])
    own_table.start()
    lax.fori_loop(1, ne, send_table, 0)

    @pl.when(edge_in)
    def _():
        spot = place(0, 0, near).at[pl.ds(0, top), pl.ds(0, EDGE)]
        pltpu.make_async_copy(edge16, spot, edge_sem.at[3]).start()

    def each(step):
        def one(e, carry):
            step(e, 2)
            return carry

        if experts > 1:
            step(0, 2)
            lax.fori_loop(1, experts - 1, one, 0)
        step(experts - 1, 1)

    def land(e, count, d):
        for fits, j in ((z >= d, z - d), (z + d < ns, z + d)):
            if isinstance(e, int) and e == 0 and d == 1:
                short = og_ref.at[0, pl.ds(0, (count - 1) * rows + edge_rows), :]
                pl.when(fits & edge_in)(lambda: wait_for(short, recv_sem.at[j, 0]))
                fits = fits & jnp.logical_not(edge_in)
            pl.when(fits)(lambda: wait_for(pieces(count), recv_sem.at[j, e]))

    def goes_on(step, d):
        return (z + d < ns) & (z > 0) if step < 0 else (z >= d) & (z < ns - 1)

    for d in range(1, ns - 1):
        def pass_on(e, count, d=d):
            land(e, count, d)
            for step in (-1, 1):
                @pl.when(goes_on(step, d))
                def _():
                    for which in range(count):
                        send_on(e, which, step, d)

        each(pass_on)

        @pl.when(inner)
        def _():
            pl.when(z >= d)(lambda: wait_for(pieces(1), last_recv.at[z - d]))
            pl.when(z + d < ns)(lambda: wait_for(pieces(1), last_recv.at[z + d]))

        for step in (-1, 1):
            send_last(step, d)

    wait_for(pieces(n), local_sem.at[0])
    wait_for(scale, own_sem.at[1])
    own_table.wait()
    for i in range(2):
        wait_for(table_ref.at[pl.ds(0, ne - 1)], table_sem.at[i])
    wait_for(column.at[pl.ds(0, ns - 1)], column_sem.at[0])
    for group, part in enumerate((first_sums, head, tail)[: 3 if experts > 1 else 2]):
        exchanged(part, group)
    for d in range(ns - 1):
        for step in (-1, 1):
            pl.when(last_goes(step, d))(lambda: wait_for(pieces(1), last_sent(step, d)))
    @pl.when(edge_in)
    def _():
        wait_for(edge16, edge_sem.at[3])

    for d in range(ns - 1):
        for step in (-1, 1):
            fits = goes_on(step, d)
            if d == 0:
                @pl.when(outward(step))
                def _():
                    wait_for(edge32, edge_sem.at[0])
                    wait_for(narrow.at[0, pl.ds(0, edge_rows)], edge_sem.at[2])
                    if n > 2:
                        wait_for(pieces(n - 2), sent(step, 0))

                fits = fits & jnp.logical_not(outward(step))
            pl.when(fits)(lambda: wait_for(pieces(n - 1), sent(step, d)))
    each(lambda e, count: land(e, count, ns - 1))


def shard_in(slot, ns):
    z = lax.axis_index("shard")
    return jnp.where(z < ns // 2, slot + 1, slot)


def move_kernel(src_ref, dst_ref):
    dst_ref[...] = src_ref[...]


def move(raw):
    block = pl.BlockSpec((1,) + raw.shape[1:], lambda i: (i, 0, 0))
    return pl.pallas_call(
        move_kernel,
        grid=(raw.shape[0],),
        out_shape=jax.ShapeDtypeStruct(raw.shape, raw.dtype),
        in_specs=[block],
        out_specs=block,
        compiler_params=pltpu.CompilerParams(vmem_limit_bytes=32 * 1024 * 1024),
        cost_estimate=pl.CostEstimate(flops=0, bytes_accessed=2 * raw.size * raw.dtype.itemsize, transcendentals=0),
    )(raw)


def move_all_kernel(ns, rows, splits, raw_ref, big_ref, small_ref, *refs):
    count = len(refs) // 2
    dst_ref, smalls, copies = refs[count], refs[:count], refs[count + 1 :]
    dst_ref[...] = raw_ref[...]
    z = lax.axis_index("shard")

    @pl.when(pl.program_id(0) == 0)
    def _():
        for small, copy in zip(smalls, copies):
            copy[...] = small[...]

    @pl.when((pl.program_id(0) == pl.num_programs(0) - 1) & (z > 0) & (z < ns - 1))
    def _():
        for ref, (lo, size) in zip((big_ref, small_ref), splits):
            for slot in range(ns - 1):
                at = pl.multiple_of(shard_in(slot, ns) * rows + lo, 16)
                dst_ref[0, pl.ds(at, size), :] = ref[slot]


def move_all(ns, rows, splits, raw, bundles, smalls):
    block = pl.BlockSpec((1,) + raw.shape[1:], lambda i: (i, 0, 0))

    def whole(x):
        return pl.BlockSpec(x.shape, lambda i: (0,) * x.ndim)

    return pl.pallas_call(
        functools.partial(move_all_kernel, ns, rows, splits),
        grid=(raw.shape[0],),
        out_shape=[jax.ShapeDtypeStruct(x.shape, x.dtype) for x in (raw, *smalls)],
        in_specs=[block] + [whole(x) for x in (*bundles, *smalls)],
        out_specs=[block] + [whole(x) for x in smalls],
        compiler_params=pltpu.CompilerParams(vmem_limit_bytes=40 * 1024 * 1024),
        cost_estimate=pl.CostEstimate(flops=0, bytes_accessed=2 * raw.size * raw.dtype.itemsize, transcendentals=0),
    )(raw, *bundles, *smalls)


def fill_kernel(ns, rows, lo, pieces_ref, whole_ref, out_ref, sem):
    z = lax.axis_index("shard")

    @pl.when((z == 0) | (z == ns - 1))
    def _():
        stores = []
        for slot in range(ns - 1):
            at = pl.multiple_of(shard_in(slot, ns) * rows + lo, 16)
            spot = out_ref.at[out_ref.shape[0] - 1, pl.ds(at, pieces_ref.shape[1]), :]
            stores.append(pltpu.make_async_copy(pieces_ref.at[slot], spot, sem.at[slot]))
        for store in stores:
            store.start()
        for store in stores:
            store.wait()


def fill(ns, rows, lo, pieces, whole):
    anywhere = pl.BlockSpec(memory_space=pl.ANY)
    size = 2 * pieces.size * pieces.dtype.itemsize
    return pl.pallas_call(
        functools.partial(fill_kernel, ns, rows, lo),
        out_shape=jax.ShapeDtypeStruct(whole.shape, whole.dtype),
        in_specs=[pl.BlockSpec(memory_space=pltpu.VMEM), anywhere],
        out_specs=anywhere,
        input_output_aliases={1: 0},
        scratch_shapes=[pltpu.SemaphoreType.DMA((ns - 1,))],
        compiler_params=pltpu.CompilerParams(vmem_limit_bytes=32 * 1024 * 1024),
        cost_estimate=pl.CostEstimate(flops=0, bytes_accessed=size, transcendentals=0),
    )(pieces, whole)


def solution(mesh):
    ns, ne = mesh.shape["shard"], mesh.shape["expert"]
    assert ns >= 4

    def per_device(w_gate, avg_gate, w_up, avg_up, mix_share, router_weight, router_gain):
        experts, rows, cols = w_gate.shape
        n = 2 * experts
        ahead = max(cols // HEAD_PARTS // 128, 1) * 128
        top = rows // 2 // 16 * 16
        assert top * EDGE % cols == 0
        large = rows * 7 // 8 // 16 * 16
        splits = ((0, large), (large, rows - large))
        dma = pltpu.SemaphoreType.DMA
        f32, bf16 = jnp.float32, jnp.bfloat16
        anywhere = pl.BlockSpec(memory_space=pl.ANY)
        serve = jax.ShapeDtypeStruct((experts, ns * rows, cols), bf16)
        scale = jax.ShapeDtypeStruct((experts, cols), f32)
        bundles = tuple(jax.ShapeDtypeStruct((ns - 1, size, cols), bf16) for _, size in splits)
        table = jax.ShapeDtypeStruct((ne, ns, experts, rows), bf16)
        raw_gate, raw_up, scale_gate, scale_up, *bundles, table = pl.pallas_call(
            functools.partial(kernel, ns, ne, experts, rows, cols, ahead, top, splits),
            out_shape=(serve, serve, scale, scale, *bundles, table),
            in_specs=[anywhere] * 7,
            out_specs=(anywhere,) * 7,
            scratch_shapes=[
                pltpu.VMEM((n, rows, cols), f32),
                pltpu.VMEM((SLOTS, rows, cols), f32),
                pltpu.VMEM((n, rows, cols), bf16),
                pltpu.VMEM((ns + 1, 1, ahead), f32),
                pltpu.VMEM((ns + 1, 2, cols), f32),
                pltpu.VMEM((ns + 1, max(n - 2, 1), cols), f32),
                pltpu.VMEM((2, experts, cols), f32),
                pltpu.SMEM((experts,), f32),
                pltpu.VMEM((experts, rows), f32),
                pltpu.VMEM((1, rows), f32),
                pltpu.VMEM((ns, experts, rows), bf16),
                pltpu.VMEM((top, EDGE), f32),
                pltpu.VMEM((top, EDGE), bf16),
                dma((SLOTS,)),
                dma((1,)),
                dma((3,)),
                dma((1,)),
                dma((ns, experts)),
                dma((ns,)),
                dma((2, ns - 1)),
                dma((2, ns - 1)),
                dma((3, 4)),
                dma((2,)),
                dma((2,)),
                dma((2,)),
                dma((4,)),
            ],
            compiler_params=pltpu.CompilerParams(
                collective_id=0, has_side_effects=True, vmem_limit_bytes=62 * 1024 * 1024
            ),
        )(mix_share, w_gate, avg_gate, w_up, avg_up, router_weight.T, router_gain.reshape(1, rows))
        pieces = [lax.ppermute(bundle, "shard", [(1, 0), (ns - 2, ns - 1)]) for bundle in bundles]
        serve_gate = move(raw_gate)
        smalls = (scale_gate, scale_up, table)
        serve_up, scale_gate, scale_up, table = move_all(ns, rows, splits, raw_up, bundles, smalls)
        for (lo, _), piece in zip(splits, pieces):
            serve_up = fill(ns, rows, lo, piece, serve_up)
        serve_router = table.transpose(1, 3, 0, 2).reshape(ns * rows, ne * experts)
        return serve_gate, serve_up, scale_gate, scale_up, serve_router

    return jax.shard_map(
        per_device,
        mesh=mesh,
        in_specs=(
            P("expert", "shard", None),
            P("expert", "shard", None),
            P("expert", "shard", None),
            P("expert", "shard", None),
            P("expert"),
            P("shard", "expert"),
            P("shard"),
        ),
        out_specs=(
            P("expert", None, None),
            P("expert", None, None),
            P("expert", None),
            P("expert", None),
            P(),
        ),
        check_vma=False,
    )
```
